512 devices in a mesh: py: 16 (over y_hi, z), px: 32 (over x, y_lo, core).
Axes of the slice: x: 4, y: 8 (y_hi: 2, y_lo: 4; y = y_hi * 4 + y_lo), z: 8, core: 2. Of those that a mesh axis runs over, the one named last changes fastest.
Arguments:
- residual: bfloat16 [16, 32, 4096, 128], P('py', 'px'), may hold values from -10 to 75
- footprints: bfloat16 [16, 32, 40, 4096], P('py', 'px'), may hold values from 0.049804688 to 1
- traces: bfloat16 [16, 32, 40, 128], P('py', 'px'), may hold values from 0.099609375 to 2
- merge_pairs: int32 [16, 32, 16, 3], P('py', 'px'), may hold values from 0 to 39, as said below
- pair_counts: int32 [16, 32], P('py', 'px'), may hold values from 1 to 16, as said below
- comp_counts: int32 [16, 32], P('py', 'px'), may hold values from 27 to 40, as said below
- row_intersections: int32 [15], replicated, may hold values from 8 to 24
- col_intersections: int32 [31], replicated, may hold values from 8 to 24
Outputs:
- new_footprints: bfloat16 [16, 32, 40, 4096], P('py', 'px')
- new_traces: bfloat16 [16, 32, 40, 128], P('py', 'px')
- correlations: float32 [16, 32, 40, 24], P('py', 'px')
The draws below stay inside these ranges and needn't reach their ends.
Inputs may be any that keep to these rules, and one draw needn't show every extreme that they name: `merge_pairs`: in slot m < pair_counts[p]: a component id i with 24 <= i < comp_counts[p], a direction d whose neighbour patch exists, and a slot s < 3; ids and (d, s) are distinct within a patch. Later slots are unused. `pair_counts`: at most 3 times the number of neighbours of the patch; some patch has 16. `comp_counts`: at least 24 + pair_counts[p]; components from comp_counts[p] on are unused; some patch has 40.
All inputs are finite; a program needn't handle non-finite values.
Results may differ from the reference program's by a relative error of at most 0.0026.
Values may be sent and summed in bfloat16 or wider, within the bound.
No kernel may reach another device: no remote copies, remote signals or barrier semaphores. Data moves between devices by JAX's collectives and lax.ppermute only.
A program may use at most 64 MiB of HBM per device.

```python
import math
import jax
import jax.numpy as jnp
from jax import lax

PH = 64
PW = 64
K = 40
NBR = 3
BORDER = 24
MP = 16
F = 128
ITERS = 4
OV_LO = 8
OV_HI = 24
GR = 16
GC = 32


def merge_layout(key):
    base_key = jax.random.fold_in(key, 7211)
    key_counts, key_codes, key_extra, key_owned = jax.random.split(base_key, 4)
    grid_row = jnp.arange(GR, dtype=jnp.int32)[:, None] + jnp.zeros((1, GC), jnp.int32)
    grid_col = jnp.arange(GC, dtype=jnp.int32)[None, :] + jnp.zeros((GR, 1), jnp.int32)
    direction = jnp.arange(8, dtype=jnp.int32)
    flat_index = direction + (direction >= 4).astype(jnp.int32)
    step_y = flat_index // 3 - 1
    step_x = flat_index % 3 - 1
    target_y = grid_row[:, :, None] + step_y
    target_x = grid_col[:, :, None] + step_x
    present = (target_y >= 0) & (target_y < GR) & (target_x >= 0) & (target_x < GC)
    capacity = jnp.minimum(NBR * jnp.sum(present.astype(jnp.int32), axis=-1), MP)
    divisor = 1 + jax.random.randint(key_counts, (GR, GC), 0, 4)
    pair_total = 1 + (capacity - 1) // divisor
    pair_total = jnp.where((grid_row == 1) & (grid_col == 1), capacity, pair_total)
    code_index = jnp.arange(BORDER, dtype=jnp.int32)
    code_present = jnp.repeat(present, NBR, axis=-1)
    code_scores = jax.random.randint(key_codes, (GR, GC, BORDER), 0, 1 << 20) * BORDER + code_index + jnp.where(code_present, 0, 1 << 26)
    chosen = jnp.argsort(code_scores, axis=-1)[:, :, :MP].astype(jnp.int32)
    extra_count = jax.random.randint(key_extra, (GR, GC), 0, K - BORDER - pair_total + 1)
    component_total = BORDER + pair_total + extra_count
    spare_index = jnp.arange(K - BORDER, dtype=jnp.int32)
    owned_scores = jax.random.randint(key_owned, (GR, GC, K - BORDER), 0, 1 << 20) * (K - BORDER) + spare_index + jnp.where(BORDER + spare_index[None, None, :] < component_total[:, :, None], 0, 1 << 26)
    owned_ids = BORDER + jnp.argsort(owned_scores, axis=-1)[:, :, :MP].astype(jnp.int32)
    pair_table = jnp.stack([owned_ids, chosen // NBR, chosen % NBR], axis=-1).astype(jnp.int32)
    return (pair_table, pair_total.astype(jnp.int32), component_total.astype(jnp.int32))


def draw_merge_pairs(key, part):
    return merge_layout(key)[0]


def draw_pair_counts(key, part):
    return merge_layout(key)[1]


def draw_comp_counts(key, part):
    return merge_layout(key)[2]


def rank_mask(key, count, chosen):
    scores = jax.random.randint(key, (GR, GC, count), 0, 1 << 30)
    ranks = jnp.argsort(jnp.argsort(scores, axis=-1), axis=-1)
    return (ranks < chosen).astype(jnp.float32)


def draw_residual(key, part):
    base_key = jax.random.fold_in(key, 5309)
    key_noise, key_pixels, key_frames, key_spatial, key_temporal = jax.random.split(base_key, 5)
    pixel_count = PH * PW
    pixel_live = max(pixel_count // 32, 1)
    frame_live = max(F // 16, 1)
    pixel_mask = rank_mask(key_pixels, pixel_count, pixel_live)
    frame_mask = rank_mask(key_frames, F, frame_live)
    spatial = jnp.exp(jax.random.uniform(key_spatial, (GR, GC, pixel_count), jnp.float32, math.log(0.05), 0.0)) * pixel_mask
    temporal = jnp.exp(jax.random.uniform(key_temporal, (GR, GC, F), jnp.float32, math.log(0.1), math.log(2.0))) * frame_mask
    noise = jnp.clip(2.0 * jax.random.normal(key_noise, (GR, GC, pixel_count, F), jnp.float32), -10.0, 10.0)
    strength = 1.2
    amplitude = strength * math.sqrt(pixel_count * F / (pixel_live * frame_live))
    values = noise + amplitude * spatial[:, :, :, None] * temporal[:, :, None, :]
    return values.astype(jnp.bfloat16)


def with_ends(values, rng, smallest, largest):
    shape = values.shape
    index_at = [jax.random.randint(jax.random.fold_in(rng, axis), (), 0, shape[axis]) for axis in range(len(shape))]
    values = values.at[tuple(index_at)].set(smallest)
    longest = shape.index(max(shape))
    index_at[longest] = (index_at[longest] + 1) % shape[longest]
    return values.at[tuple(index_at)].set(largest)


def block_scale(own_key, shape, cuts, least, top_value):
    def one(position, shards_of):
        heights = jax.random.uniform(jax.random.fold_in(jax.random.fold_in(own_key, 6), position), (shards_of,), jnp.float32, least / len(cuts), top_value / len(cuts))
        return jnp.repeat(jnp.exp(heights), shape[position] // shards_of).reshape((-1,) + (1,) * (len(shape) - position - 1))

    factor_of = one(*cuts[0])
    for cut in cuts[1:]:
        factor_of = factor_of * one(*cut)
    return factor_of


def setup_inputs(seed: int = 0) -> dict:
    splits = jax.random.split(jax.random.key(seed), 9)
    residual = draw_residual(jax.random.fold_in(splits[8], 71), 0)
    footprints = jnp.clip(jnp.exp(math.log(1.0) - 2.9996462 * jax.random.uniform(splits[1], (GR, GC, K, PH * PW), jnp.float32) ** block_scale(splits[1], (GR, GC, K, PH * PW), ((0, 16), (1, 32)), -0.2, 0.2)), 0.049804688, 1.0).astype(jnp.bfloat16)
    traces = jnp.clip(jnp.exp(math.log(2.0) - 2.9996462 * jax.random.uniform(splits[2], (GR, GC, K, F), jnp.float32) ** block_scale(splits[2], (GR, GC, K, F), ((0, 16), (1, 32)), -0.2, 0.2)), 0.099609375, 2.0).astype(jnp.bfloat16)
    merge_pairs = draw_merge_pairs(jax.random.fold_in(splits[8], 71), 0)
    pair_counts = draw_pair_counts(jax.random.fold_in(splits[8], 71), 0)
    comp_counts = draw_comp_counts(jax.random.fold_in(splits[8], 71), 0)
    row_intersections = with_ends(jax.random.randint(splits[6], (GR - 1,), OV_LO, OV_HI + 1), jax.random.fold_in(splits[6], 1), OV_LO, OV_HI).astype(jnp.int32)
    col_intersections = with_ends(jax.random.randint(splits[7], (GC - 1,), OV_LO, OV_HI + 1), jax.random.fold_in(splits[7], 1), OV_LO, OV_HI).astype(jnp.int32)
    return {"residual": residual, "footprints": footprints, "traces": traces, "merge_pairs": merge_pairs, "pair_counts": pair_counts, "comp_counts": comp_counts, "row_intersections": row_intersections, "col_intersections": col_intersections}


epsilon = 1e-05

def direction_steps(direction):
    flat_index = direction + (direction >= 4).astype(jnp.int32)
    return (flat_index // 3 - 1, flat_index % 3 - 1)

def lookup_table(table, index):
    places = jnp.arange(table.shape[0], dtype=jnp.int32)
    return lax.optimization_barrier(jnp.sum(jnp.where(places[None, :] == index[:, None], table[None, :], 0), axis=1)).astype(jnp.int32)

def pair_offsets(direction, grid_row, grid_col, row_intersections, col_intersections):
    step_y, step_x = direction_steps(direction)
    band_y = jnp.clip(grid_row + jnp.minimum(step_y, 0), 0, row_intersections.shape[0] - 1)
    band_x = jnp.clip(grid_col + jnp.minimum(step_x, 0), 0, col_intersections.shape[0] - 1)
    shift_y = step_y * (PH - lookup_table(row_intersections, band_y))
    shift_x = step_x * (PW - lookup_table(col_intersections, band_x))
    return (shift_y, shift_x)

def move_pixels(values, shift_y, shift_x, filler):
    pixels = jnp.arange(PH * PW, dtype=jnp.int32)
    source_y = pixels[None, :] // PW - shift_y[:, None]
    source_x = pixels[None, :] % PW - shift_x[:, None]
    inside = (source_y >= 0) & (source_y < PH) & (source_x >= 0) & (source_x < PW)
    source = jnp.clip(source_y, 0, PH - 1) * PW + jnp.clip(source_x, 0, PW - 1)
    taken = jnp.take_along_axis(values, source, axis=1)
    return jnp.where(inside, taken, filler)

def refit_pairs(residue, own_footprints, own_traces, pair_table, pair_total, border, grid_row, grid_col, row_intersections, col_intersections):
    pixel_count = PH * PW
    owned_ids = pair_table[:, 0]
    direction = pair_table[:, 1]
    border_index = NBR * direction + pair_table[:, 2]
    in_use = jnp.arange(MP, dtype=jnp.int32) < pair_total
    a_own = jnp.take(own_footprints, owned_ids, axis=0).astype(jnp.float32)
    c_own = jnp.take(own_traces, owned_ids, axis=0).astype(jnp.float32)
    remote = jnp.take(border, border_index, axis=0)
    a_remote_raw = remote[:, :pixel_count].astype(jnp.float32)
    c_remote = remote[:, pixel_count:].astype(jnp.float32)
    shift_y, shift_x = pair_offsets(direction, grid_row, grid_col, row_intersections, col_intersections)
    a_remote = move_pixels(a_remote_raw, shift_y, shift_x, 0.0)
    trace_now = c_own
    shape_now = a_own
    for iteration in range(ITERS):
        across = jnp.dot(trace_now.astype(jnp.bfloat16), residue.T, preferred_element_type=jnp.float32)
        across = across + a_own * lax.optimization_barrier(jnp.sum(c_own * trace_now, axis=1, keepdims=True)) + a_remote * lax.optimization_barrier(jnp.sum(c_remote * trace_now, axis=1, keepdims=True))
        shape_now = jnp.maximum(across, 0.0) / (lax.optimization_barrier(jnp.sum(trace_now * trace_now, axis=1, keepdims=True)) + epsilon * F)
        downward = jnp.dot(shape_now.astype(jnp.bfloat16), residue, preferred_element_type=jnp.float32)
        downward = downward + c_own * lax.optimization_barrier(jnp.sum(a_own * shape_now, axis=1, keepdims=True)) + c_remote * lax.optimization_barrier(jnp.sum(a_remote * shape_now, axis=1, keepdims=True))
        trace_now = jnp.maximum(downward, 0.0) / (lax.optimization_barrier(jnp.sum(shape_now * shape_now, axis=1, keepdims=True)) + epsilon * pixel_count)
    footprint_out = shape_now.astype(jnp.bfloat16)
    trace_out = trace_now.astype(jnp.bfloat16)
    remote_new = move_pixels(footprint_out.astype(jnp.float32), -shift_y, -shift_x, a_remote_raw).astype(jnp.bfloat16)
    owner_hot = ((owned_ids[None, :] == jnp.arange(K, dtype=jnp.int32)[:, None]) & in_use[None, :]).astype(jnp.float32)
    owner_hit = lax.optimization_barrier(jnp.sum(owner_hot, axis=1)) > 0
    new_foot = jnp.where(owner_hit[:, None], jnp.dot(owner_hot, footprint_out.astype(jnp.float32), precision=lax.Precision.HIGHEST), own_footprints.astype(jnp.float32)).astype(jnp.bfloat16)
    new_trace = jnp.where(owner_hit[:, None], jnp.dot(owner_hot, trace_out.astype(jnp.float32), precision=lax.Precision.HIGHEST), own_traces.astype(jnp.float32)).astype(jnp.bfloat16)
    border_hot = ((border_index[None, :] == jnp.arange(BORDER, dtype=jnp.int32)[:, None]) & in_use[None, :]).astype(jnp.float32)
    border_hit = lax.optimization_barrier(jnp.sum(border_hot, axis=1)) > 0
    sending = jnp.concatenate([remote_new, trace_out], axis=1).astype(jnp.float32)
    outgoing = jnp.where(border_hit[:, None], jnp.dot(border_hot, sending, precision=lax.Precision.HIGHEST), border.astype(jnp.float32)).astype(jnp.bfloat16)
    return (new_foot, new_trace, outgoing)

def neighbour_rows(block):
    padded = jnp.pad(block, ((1, 1), (1, 1), (0, 0), (0, 0)))
    pieces = []
    for direction in range(8):
        flat_index = direction + (1 if direction >= 4 else 0)
        step_y = flat_index // 3 - 1
        step_x = flat_index % 3 - 1
        source = NBR * (7 - direction)
        pieces.append(padded[1 + step_y:1 + step_y + GR, 1 + step_x:1 + step_x + GC, source:source + NBR])
    return jnp.concatenate(pieces, axis=2)

def neighbour_exists(grid_row, grid_col):
    flags = []
    for direction in range(8):
        flat_index = direction + (1 if direction >= 4 else 0)
        target_y = grid_row + flat_index // 3 - 1
        target_x = grid_col + flat_index % 3 - 1
        flags.append((target_y >= 0) & (target_y < GR) & (target_x >= 0) & (target_x < GC))
    return jnp.repeat(jnp.stack(flags, axis=-1), NBR, axis=-1)

def reference(residual, footprints, traces, merge_pairs, pair_counts, comp_counts, row_intersections, col_intersections):
    pixel_count = PH * PW
    patches = GR * GC
    packed = jnp.concatenate([footprints[:, :, :BORDER], traces[:, :, :BORDER]], axis=3)
    border = neighbour_rows(packed)
    local = traces.astype(jnp.float32)
    local = local - lax.optimization_barrier(jnp.mean(local, axis=-1, keepdims=True))
    remote = border[:, :, :, pixel_count:].astype(jnp.float32)
    remote = remote - lax.optimization_barrier(jnp.mean(remote, axis=-1, keepdims=True))
    covariance = jnp.einsum('rckf,rcbf->rckb', local, remote, precision=lax.Precision.HIGHEST) / F
    spread_local = lax.optimization_barrier(jnp.mean(local * local, axis=-1))
    spread_remote = lax.optimization_barrier(jnp.mean(remote * remote, axis=-1))
    correlation = covariance / jnp.sqrt((spread_local[..., :, None] + epsilon) * (spread_remote[..., None, :] + epsilon))
    flat_rows = jnp.arange(patches, dtype=jnp.int32) // GC
    flat_cols = jnp.arange(patches, dtype=jnp.int32) % GC

    def one_patch(items):
        residue, own_footprints, own_traces, pair_table, pair_total, border_block, grid_row, grid_col = items
        return refit_pairs(residue, own_footprints, own_traces, pair_table, pair_total, border_block, grid_row, grid_col, row_intersections, col_intersections)
    new_foot, new_trace, outgoing = lax.map(one_patch, (residual.reshape(patches, pixel_count, F), footprints.reshape(patches, K, pixel_count), traces.reshape(patches, K, F), merge_pairs.reshape(patches, MP, 3), pair_counts.reshape(patches), border.reshape(patches, BORDER, pixel_count + F), flat_rows, flat_cols))
    returned = neighbour_rows(outgoing.reshape(GR, GC, BORDER, pixel_count + F))
    new_foot = new_foot.reshape(GR, GC, K, pixel_count)
    new_trace = new_trace.reshape(GR, GC, K, F)
    grid_row = jnp.arange(GR, dtype=jnp.int32)[:, None] + jnp.zeros((1, GC), jnp.int32)
    grid_col = jnp.arange(GC, dtype=jnp.int32)[None, :] + jnp.zeros((GR, 1), jnp.int32)
    exists = neighbour_exists(grid_row, grid_col)
    reserved_foot = jnp.where(exists[..., None], returned[..., :pixel_count], new_foot[:, :, :BORDER])
    reserved_trace = jnp.where(exists[..., None], returned[..., pixel_count:], new_trace[:, :, :BORDER])
    alive = jnp.arange(K, dtype=jnp.int32)[None, None, :] < comp_counts[..., None]
    zero_value = jnp.zeros((), jnp.bfloat16)
    new_footprints = jnp.where(alive[..., None], jnp.concatenate([reserved_foot, new_foot[:, :, BORDER:]], axis=2), zero_value)
    new_traces = jnp.where(alive[..., None], jnp.concatenate([reserved_trace, new_trace[:, :, BORDER:]], axis=2), zero_value)
    correlations = jnp.where(alive[..., None], correlation, 0.0)
    return (new_footprints, new_traces, correlations)
```

```python
import jax
import jax.numpy as jnp
from jax import lax
from jax.experimental import pallas as pl
from jax.experimental.pallas import tpu as pltpu
from jax.sharding import PartitionSpec as P

PH = 64
PW = 64
NPIX = PH * PW
K = 40
NBR = 3
BORDER = 24
MP = 16
F = 128
ITERS = 4
OV_HI = 24
epsilon = 1e-05

BAND = OV_HI * PW
LOW = NPIX - BAND
CW = BAND // 4
EW = 896
XW = 2 * CW + EW
YW = 3 * CW
CH = 128
PAD = 9
PBW = (PAD + 12 + PAD) * CH

f32 = jnp.float32
bf16 = jnp.bfloat16


def iota(shape, dim):
    return lax.broadcasted_iota(jnp.int32, shape, dim)


def sides():
    row = lax.axis_index("py")
    col = lax.axis_index("px")
    sy = 1 - 2 * lax.rem(row, 2)
    sx = 1 - 2 * lax.rem(col, 2)
    return row, col, (sy, -sy), (sx, -sx)


def direction(dy, dx):
    flat = (dy + 1) * 3 + dx + 1
    return flat - (flat > 4).astype(jnp.int32) if not isinstance(flat, int) else flat - (flat > 4)


def hot(mask):
    return jnp.where(mask, 1.0, 0.0).astype(bf16)


def dot(a, b):
    return jnp.dot(a, b, preferred_element_type=f32)


def band_start(dy):
    return jnp.where(dy > 0, LOW, 0)


def pack_rows(pick, pieces, tail, width):
    return dot(pick, jnp.concatenate(pieces + [tail], axis=0)).astype(bf16)


def pixel_shift(dy, dx, row, col, row_ref, col_ref, rows, cols):
    ri = row_ref[jnp.clip(row + jnp.minimum(dy, 0), 0, rows - 2)]
    ci = col_ref[jnp.clip(col + jnp.minimum(dx, 0), 0, cols - 2)]
    return dy * (OV_HI - ri), dx * (PW - ci), ri, ci


def column_matrix(ox):
    i = iota((CH, CH), 0)
    o = iota((CH, CH), 1)
    x = (o & (PW - 1)) - ox
    return hot((i == o - ox) & (x >= 0) & (x < PW))


def band_matrix(odd, ox):
    i = iota((2 * CH, CH), 0)
    o = iota((2 * CH, CH), 1)
    x = (o & (PW - 1)) - ox
    return hot((i == o + CH - PW * odd - ox) & (x >= 0) & (x < PW))


def place_band(pbuf, at, band, shift, ox, rows):
    pbuf[at, :, PAD * CH : PAD * CH + BAND] = band.astype(bf16)
    chunks = shift >> 1
    first = pl.multiple_of((PAD - 1 - chunks) * CH, CH)
    stack = jnp.concatenate(
        [pbuf[at, :, pl.ds(pl.multiple_of(first + CH * m, CH), 2 * CH)] for m in range(12)], axis=0
    )
    return dot(stack, band_matrix(shift & 1, ox))


def place_whole(whole, ox, rows):
    stack = jnp.concatenate(
        [whole[:, CH * m : CH * (m + 1)] for m in range(32)], axis=0
    ).astype(bf16)
    return dot(stack, column_matrix(ox))


def receive(select, n, xs, ys, acc, pbuf, row, col, sy, sx, row_ref, col_ref, rows, cols):
    pbuf[...] = jnp.zeros(pbuf.shape, bf16)
    tail = jnp.zeros((n, 2 * CH), f32)
    whole = None
    for t in range(2):
        picked = dot(select(direction(0, sx[t])), xs[t][:, 2 * CW : XW])
        full = jnp.concatenate(
            [picked[n * g : n * (g + 1)] for g in range(4)] + [picked[4 * n :, 0:512]], axis=1
        )
        tail = tail + picked[4 * n :, 512 : 512 + 2 * CH]
        _, ox, _, _ = pixel_shift(0, sx[t], row, col, row_ref, col_ref, rows, cols)
        moved = place_whole(full, ox, n)
        whole = moved if whole is None else whole + moved
    for m in range(32):
        acc[:, CH * m : CH * (m + 1)] = whole[n * m : n * (m + 1)]
    for u in range(2):
        moved = None
        for j, dx in enumerate((0, sx[0], sx[1])):
            picked = dot(select(direction(sy[u], dx)), ys[u][:, CW * j : CW * (j + 1)])
            band = jnp.concatenate([picked[n * g : n * (g + 1)] for g in range(4)], axis=1)
            tail = tail + picked[4 * n :, 0 : 2 * CH]
            shift, ox, _, _ = pixel_shift(sy[u], dx, row, col, row_ref, col_ref, rows, cols)
            one = place_band(pbuf, 3 * u + j, band, shift, ox, n)
            moved = one if moved is None else moved + one
        start = band_start(sy[u])
        for m in range(12):
            lanes = pl.ds(pl.multiple_of(start + CH * m, CH), CH)
            acc[:, lanes] += moved[n * m : n * (m + 1)]
    return tail


def send_all(pick, src, tail_narrow, tail_wide, outs, sy, sx):
    xa, xb, va, vb = outs

    def band_seg(dy, dx):
        start = band_start(dy)
        pieces = [
            src[:, pl.ds(pl.multiple_of(start + CW * g, CH), CW)] for g in range(4)
        ]
        return pack_rows(pick(direction(dy, dx)), pieces, tail_narrow, CW)

    def whole_seg(dx):
        pieces = [src[:, EW * g : EW * (g + 1)] for g in range(4)]
        last = jnp.concatenate([src[:, 4 * EW : NPIX], tail_wide], axis=1)
        return pack_rows(pick(direction(0, dx)), pieces, last, EW)

    for t, out in enumerate((xa, xb)):
        out[:, 0:CW] = band_seg(sy[0], sx[t])
        out[:, CW : 2 * CW] = band_seg(sy[1], sx[t])
        out[:, 2 * CW : XW] = whole_seg(sx[t])
    va[...] = band_seg(sy[0], 0)
    vb[...] = band_seg(sy[1], 0)


def group_of(j):
    g = (j >= 3).astype(jnp.int32) + (j >= 6) + (j >= 9) + (j >= 12)
    return g, j - 3 * g


def pack_kernel(foot, tr, xa, xb, va, vb, src):
    _, _, sy, sx = sides()
    src[...] = foot[0:32, :]
    trace = tr[0:32, :]
    blank = jnp.zeros((32, 2 * CH), bf16)
    tail = jnp.concatenate([trace, blank], axis=1)
    j = iota((16, 160), 0)
    kk = iota((16, 160), 1)
    g, s = group_of(j)
    same = ((kk >> 5) == g) & (j < 15)
    comp = (kk & 31) - s

    def pick(d):
        return hot(same & (comp == 3 * d))

    send_all(pick, src, tail, tail, (xa, xb, va, vb), sy, sx)


def slot_masks(table, total):
    own = table[:, 0:1]
    idx = NBR * table[:, 1:2] + table[:, 2:3]
    live = iota((MP, 1), 0) < total
    return own, idx, live


def refit_kernel(
    rows, cols, count, row_ref, col_ref, res, foot, tr, table, wide, rxa, rxb, rya, ryb,
    xa, xb, va, vb, merged, mtrace, acc, own, pbuf,
):
    row, col, sy, sx = sides()
    total = count[0, 0]
    ids, idx, live = slot_masks(table, total)
    own_hot = hot(ids == iota((MP, K), 1))
    own[...] = dot(own_hot, foot[...])
    c_own = dot(own_hot, tr[...])
    j5 = iota((5 * MP, 16), 1)
    g5 = iota((5 * MP, 16), 0) >> 4
    s5 = j5 - 3 * g5
    idx5 = jnp.concatenate([jnp.where(live, idx, -100)] * 5, axis=0)
    fits = (s5 >= 0) & (s5 < 3)

    def select(d):
        return hot(fits & (idx5 == 3 * d + s5))

    tail = receive(
        select, MP, (rxa, rxb), (rya, ryb), acc, pbuf, row, col, sy, sx, row_ref, col_ref, rows, cols
    )
    c_rem = tail[:, 0:F]
    trace = c_own
    step = 512
    for it in range(ITERS):
        tb = trace.astype(bf16)
        co = jnp.sum(c_own * trace, axis=1, keepdims=True)
        cr = jnp.sum(c_rem * trace, axis=1, keepdims=True)
        scale = 1.0 / (jnp.sum(trace * trace, axis=1, keepdims=True) + epsilon * F)
        down = jnp.zeros((MP, F), f32)
        sa = jnp.zeros((MP, CH), f32)
        sr = jnp.zeros((MP, CH), f32)
        ss = jnp.zeros((MP, CH), f32)
        for n in range(NPIX // step):
            lanes = slice(step * n, step * (n + 1))
            part = res[lanes, :]
            across = lax.dot_general(
                tb, part, (((1,), (1,)), ((), ())), preferred_element_type=f32
            )
            ao = own[:, lanes]
            ar = acc[:, lanes]
            now = jnp.maximum(across + ao * co + ar * cr, 0.0) * scale
            nb = now.astype(bf16)
            if it == ITERS - 1:
                merged[:, lanes] = jnp.where(live, now, 0.0).astype(bf16)
            down = down + dot(nb, part)
            pa = ao * now
            pr = ar * now
            ps = now * now
            for q in range(step // CH):
                cut = slice(CH * q, CH * (q + 1))
                sa = sa + pa[:, cut]
                sr = sr + pr[:, cut]
                ss = ss + ps[:, cut]
        down = (
            down
            + c_own * jnp.sum(sa, axis=1, keepdims=True)
            + c_rem * jnp.sum(sr, axis=1, keepdims=True)
        )
        trace = jnp.maximum(down, 0.0) / (jnp.sum(ss, axis=1, keepdims=True) + epsilon * NPIX)
    tout = jnp.where(live, trace, 0.0).astype(bf16)
    mtrace[...] = tout
    j = iota((16, 5 * MP), 0)
    kk = iota((16, 5 * MP), 1)
    g, s = group_of(j)
    slot = kk & 15
    same = ((kk >> 4) == g) & (j < 15) & (slot < total)
    comp = NBR * wide[1:2, :] + wide[2:3, :] - s

    def pick(d):
        return hot(same & (comp == 3 * d))

    ones = jnp.ones((MP, CH), bf16)
    blank = jnp.zeros((MP, CH), bf16)
    tail = jnp.concatenate([tout, ones, blank], axis=1)
    send_all(pick, merged, tail, tail, (xa, xb, va, vb), sy, sx)


def corr_kernel(comp, tr, rxa, rxb, rya, ryb, out):
    _, _, sy, sx = sides()
    k = iota((BORDER, 16), 0)
    j = iota((BORDER, 16), 1)
    s = j - 12
    fits = (s >= 0) & (s < 3)
    z = jnp.zeros((BORDER, F), f32)
    for t, ref in enumerate((rxa, rxb)):
        at = 2 * CW + 512
        z = z + dot(hot(fits & (k == 3 * direction(0, sx[t]) + s)), ref[:, at : at + F])
    for u, ref in enumerate((rya, ryb)):
        for q, dx in enumerate((0, sx[0], sx[1])):
            z = z + dot(hot(fits & (k == 3 * direction(sy[u], dx) + s)), ref[:, CW * q : CW * q + F])
    x = tr[...].astype(f32)
    x = x - jnp.mean(x, axis=1, keepdims=True)
    z = z - jnp.mean(z, axis=1, keepdims=True)
    nt = (((1,), (1,)), ((), ()))
    cov = lax.dot_general(x, z, nt, precision=lax.Precision.HIGHEST, preferred_element_type=f32) / F
    vx = jnp.mean(x * x, axis=1, keepdims=True)
    vz = lax.dot_general(
        jnp.ones((8, F), f32), z * z, nt, precision=lax.Precision.HIGHEST, preferred_element_type=f32
    )[0:1] / F
    alive = iota((K, 1), 0) < comp[0, 0]
    out[...] = jnp.where(alive, cov / jnp.sqrt((vx + epsilon) * (vz + epsilon)), 0.0)


def final_kernel(
    rows, cols, count, compc, row_ref, col_ref, foot, tr, wide, merged, mtrace, rxa, rxb, rya, ryb,
    nfoot, ntrace, acc, pbuf,
):
    row, col, sy, sx = sides()
    n = 32
    j5 = iota((5 * n, 16), 1)
    r5 = iota((5 * n, 16), 0)
    s5 = j5 - 3 * (r5 >> 5)
    k5 = r5 & 31
    fits = (s5 >= 0) & (s5 < 3)

    def select(d):
        return hot(fits & (k5 == 3 * d + s5))

    tail = receive(
        select, n, (rxa, rxb), (rya, ryb), acc, pbuf, row, col, sy, sx, row_ref, col_ref, rows, cols
    )
    flag = tail[0:BORDER, CH : CH + 1] > 0.5
    k = iota((BORDER, 1), 0)
    up = k < 9
    down = k >= 15
    left = (k < 3) | ((k >= 9) & (k < 12)) | ((k >= 15) & (k < 18))
    right = ((k >= 6) & (k < 9)) | ((k >= 12) & (k < 15)) | (k >= 21)
    _, _, r_up, _ = pixel_shift(-1, 0, row, col, row_ref, col_ref, rows, cols)
    _, _, r_dn, _ = pixel_shift(1, 0, row, col, row_ref, col_ref, rows, cols)
    _, _, _, c_lf = pixel_shift(0, -1, row, col, row_ref, col_ref, rows, cols)
    _, _, _, c_rt = pixel_shift(0, 1, row, col, row_ref, col_ref, rows, cols)
    y_lo = jnp.where(down, PH - r_dn, 0)
    y_hi = jnp.where(flag, jnp.where(up, r_up, PH), 0)
    x_lo = jnp.where(right, PW - c_rt, 0)
    x_hi = jnp.where(left, c_lf, PW)
    total = count[0, 0]
    own_id = wide[0:1, 0:MP]
    own_mask = (iota((K - BORDER, MP), 0) + BORDER == own_id) & (iota((K - BORDER, MP), 1) < total)
    own_hot = hot(own_mask)
    hit = jnp.sum(own_hot.astype(f32), axis=1, keepdims=True) > 0.5
    alive = iota((K - BORDER, 1), 0) + BORDER < compc[0, 0]
    step = 512
    for b in range(NPIX // step):
        lanes = slice(step * b, step * (b + 1))
        pix = iota((1, step), 1) + step * b
        y = pix >> 6
        x = pix & (PW - 1)
        mine = foot[:, lanes].astype(f32)
        inside = (y >= y_lo) & (y < y_hi) & (x >= x_lo) & (x < x_hi)
        top = jnp.where(inside, acc[0:BORDER, lanes], mine[0:BORDER])
        got = dot(own_hot, merged[:, lanes])
        low = jnp.where(alive, jnp.where(hit, got, mine[BORDER:]), 0.0)
        nfoot[:, lanes] = jnp.concatenate([top, low], axis=0).astype(bf16)
    mine = tr[...].astype(f32)
    top = jnp.where(flag, tail[0:BORDER, 0:F], mine[0:BORDER])
    low = jnp.where(alive, jnp.where(hit, dot(own_hot, mtrace[...]), mine[BORDER:]), 0.0)
    ntrace[...] = jnp.concatenate([top, low], axis=0).astype(bf16)


SMEM = pl.BlockSpec(memory_space=pltpu.SMEM)
VMEM = pl.BlockSpec(memory_space=pltpu.VMEM)
LIMIT = 24 * 1024 * 1024


def shape(*dims, dtype=bf16):
    return jax.ShapeDtypeStruct(dims, dtype)


PACKETS = (shape(16, XW), shape(16, XW), shape(16, CW), shape(16, CW))


def call(kernel, outs, scalars, arrays, scratch, flops, name):
    return pl.pallas_call(
        kernel,
        out_shape=outs,
        in_specs=[SMEM] * scalars + [VMEM] * arrays,
        out_specs=jax.tree.map(lambda _: VMEM, outs),
        scratch_shapes=scratch,
        compiler_params=pltpu.CompilerParams(vmem_limit_bytes=LIMIT),
        cost_estimate=pl.CostEstimate(flops=flops, bytes_accessed=1 << 20, transcendentals=0),
        name=name,
    )


def swap(value, axis, parity):
    count = lax.axis_size(axis)
    pairs = []
    for i in range(parity, count - 1, 2):
        pairs += [(i, i + 1), (i + 1, i)]
    return lax.ppermute(value, axis, pairs)


def exchange(xa, xb, va, vb):
    rxb = swap(xb, "px", 1)
    rxa = swap(xa, "px", 0)
    yb = jnp.concatenate([vb, rxa[:, CW : 2 * CW], rxb[:, CW : 2 * CW]], axis=1)
    ya = jnp.concatenate([va, rxa[:, 0:CW], rxb[:, 0:CW]], axis=1)
    ryb = swap(yb, "py", 1)
    rya = swap(ya, "py", 0)
    return rxa, rxb, rya, ryb


def shards(
    residual, footprints, traces, merge_pairs, pair_counts, comp_counts, row_inter, col_inter
):
    res = residual[0, 0]
    foot = footprints[0, 0]
    tr = traces[0, 0]
    table = merge_pairs[0, 0]
    wide = jnp.tile(table.T, (1, 5))
    rows, cols = lax.axis_size("py"), lax.axis_size("px")

    packets = call(
        pack_kernel, PACKETS, 0, 2, [pltpu.VMEM((32, NPIX), bf16)], 1 << 24, "pack"
    )(foot, tr)
    got = exchange(*packets)

    def refit(*refs):
        refit_kernel(rows, cols, *refs)

    xa, xb, va, vb, merged, mtrace = call(
        refit,
        PACKETS + (shape(MP, NPIX), shape(MP, F)),
        3,
        9,
        [
            pltpu.VMEM((MP, NPIX), f32),
            pltpu.VMEM((MP, NPIX), f32),
            pltpu.VMEM((6, MP, PBW), bf16),
        ],
        1 << 28,
        "refit",
    )(pair_counts, row_inter, col_inter, res, foot, tr, table, wide, *got)
    back = exchange(xa, xb, va, vb)

    corr = call(corr_kernel, shape(K, BORDER, dtype=f32), 1, 5, [], 1 << 22, "corr")(
        comp_counts, tr, *got
    )

    def final(*refs):
        final_kernel(rows, cols, *refs)

    nfoot, ntrace = call(
        final,
        (shape(K, NPIX), shape(K, F)),
        4,
        9,
        [pltpu.VMEM((32, NPIX), f32), pltpu.VMEM((6, 32, PBW), bf16)],
        1 << 26,
        "final",
    )(pair_counts, comp_counts, row_inter, col_inter, foot, tr, wide, merged, mtrace, *back)
    return nfoot[None, None], ntrace[None, None], corr[None, None]


def solution(mesh):
    in_specs = (
        P("py", "px", None, None),
        P("py", "px", None, None),
        P("py", "px", None, None),
        P("py", "px", None, None),
        P("py", "px"),
        P("py", "px"),
        P(),
        P(),
    )
    out_specs = (P("py", "px", None, None), P("py", "px", None, None), P("py", "px", None, None))
    return jax.shard_map(shards, mesh=mesh, in_specs=in_specs, out_specs=out_specs, check_vma=False)
```

```python
import jax
import jax.numpy as jnp
from jax import lax
from jax.experimental import pallas as pl
from jax.experimental.pallas import tpu as pltpu
from jax.sharding import PartitionSpec as P


PH = 64
PW = 64
NPIX = PH * PW
K = 40
NBR = 3
BORDER = 24
MP = 16
F = 128
ITERS = 4
OV_HI = 24
epsilon = 1e-05

BAND = OV_HI * PW
LOW = NPIX - BAND
CW = BAND // 4
EW = 896
XW = 2 * CW + EW
CH = 128
PAD = 9
PBW = (PAD + 12 + PAD) * CH

f32 = jnp.float32
bf16 = jnp.bfloat16


def iota(shape, dim):
    return lax.broadcasted_iota(jnp.int32, shape, dim)


def sides():
    row = lax.axis_index("py")
    col = lax.axis_index("px")
    sy = 1 - 2 * lax.rem(row, 2)
    sx = 1 - 2 * lax.rem(col, 2)
    return row, col, (sy, -sy), (sx, -sx)


def direction(dy, dx):
    flat = (dy + 1) * 3 + dx + 1
    return flat - (flat > 4).astype(jnp.int32) if not isinstance(flat, int) else flat - (flat > 4)


def hot(mask):
    return jnp.where(mask, 1.0, 0.0).astype(bf16)


def dot(a, b):
    return jnp.dot(a, b, preferred_element_type=f32)


def band_start(dy):
    return jnp.where(dy > 0, LOW, 0)


def pack_rows(pick, pieces, tail):
    return dot(pick, jnp.concatenate(pieces + [tail], axis=0)).astype(bf16)


def pixel_shift(dy, dx, row, col, row_ref, col_ref, rows, cols):
    ri = row_ref[jnp.clip(row + jnp.minimum(dy, 0), 0, rows - 2)]
    ci = col_ref[jnp.clip(col + jnp.minimum(dx, 0), 0, cols - 2)]
    return dy * (OV_HI - ri), dx * (PW - ci), ri, ci


def column_matrix(ox):
    i = iota((CH, CH), 0)
    o = iota((CH, CH), 1)
    x = (o & (PW - 1)) - ox
    return hot((i == o - ox) & (x >= 0) & (x < PW))


def band_matrix(odd, ox):
    i = iota((2 * CH, CH), 0)
    o = iota((2 * CH, CH), 1)
    x = (o & (PW - 1)) - ox
    return hot((i == o + CH - PW * odd - ox) & (x >= 0) & (x < PW))


def place_whole(whole, ox):
    stack = jnp.concatenate(
        [whole[:, CH * m : CH * (m + 1)] for m in range(32)], axis=0
    ).astype(bf16)
    return dot(stack, column_matrix(ox))


def receive_sides(select, n, xs, row, col, sx, row_ref, col_ref, rows, cols):
    tail = jnp.zeros((n, 2 * CH), f32)
    whole = None
    for t in range(2):
        picked = dot(select(direction(0, sx[t])), xs[t][:, 2 * CW : XW])
        full = jnp.concatenate(
            [picked[n * g : n * (g + 1)] for g in range(4)] + [picked[4 * n :, 0:512]], axis=1
        )
        tail = tail + picked[4 * n :, 512 : 512 + 2 * CH]
        _, ox, _, _ = pixel_shift(0, sx[t], row, col, row_ref, col_ref, rows, cols)
        moved = place_whole(full, ox)
        whole = moved if whole is None else whole + moved
    return whole, tail


def clear_pads(pbuf):
    pbuf[:, :, 0 : PAD * CH] = jnp.zeros(pbuf.shape[:2] + (PAD * CH,), bf16)
    pbuf[:, :, PAD * CH + BAND :] = jnp.zeros(pbuf.shape[:2] + (PBW - PAD * CH - BAND,), bf16)


def receive_bands(selects, n, ys, pbuf, row, col, sy, sx, row_ref, col_ref, rows, cols, ready):
    steps = (0, sx[0], sx[1])
    picked = [
        [
            dot(selects[u](direction(sy[u], dx)), ys[u][:, CW * j : CW * (j + 1)])
            for j, dx in enumerate(steps)
        ]
        for u in range(2)
    ]
    ready()
    clear_pads(pbuf)
    for u in range(2):
        for j in range(3):
            for g in range(4):
                at = PAD * CH + CW * g
                pbuf[3 * u + j, :, at : at + CW] = picked[u][j][n * g : n * (g + 1)].astype(bf16)
    out = []
    for u in range(2):
        moved = None
        tail = jnp.zeros((n, 2 * CH), f32)
        for j, dx in enumerate(steps):
            shift, ox, _, _ = pixel_shift(sy[u], dx, row, col, row_ref, col_ref, rows, cols)
            first = (PAD - 1 - (shift >> 1)) * CH
            stack = jnp.concatenate(
                [
                    pbuf[3 * u + j, :, pl.ds(pl.multiple_of(first + CH * m, CH), 2 * CH)]
                    for m in range(12)
                ],
                axis=0,
            )
            one = dot(stack, band_matrix(shift & 1, ox))
            moved = one if moved is None else moved + one
            tail = tail + picked[u][j][4 * n :, 0 : 2 * CH]
        out.append((moved, tail))
    return out


def fetch(row_in, col_in, row_ref, col_ref, sem):
    loads = (
        pltpu.make_async_copy(row_in, row_ref, sem.at[0]),
        pltpu.make_async_copy(col_in, col_ref, sem.at[1]),
    )
    for load in loads:
        load.start()

    def ready():
        for load in loads:
            load.wait()

    return ready


def send_all(pick, src, tail_narrow, tail_wide, outs, sy, sx):
    xa, xb, va, vb = outs

    def band_seg(dy, dx):
        start = band_start(dy)
        pieces = [
            src[:, pl.ds(pl.multiple_of(start + CW * g, CH), CW)] for g in range(4)
        ]
        return pack_rows(pick(direction(dy, dx)), pieces, tail_narrow)

    def whole_seg(dx):
        pieces = [src[:, EW * g : EW * (g + 1)] for g in range(4)]
        last = jnp.concatenate([src[:, 4 * EW : NPIX], tail_wide], axis=1)
        return pack_rows(pick(direction(0, dx)), pieces, last)

    for t, out in enumerate((xa, xb)):
        out[:, 0:CW] = band_seg(sy[0], sx[t])
        out[:, CW : 2 * CW] = band_seg(sy[1], sx[t])
        out[:, 2 * CW : XW] = whole_seg(sx[t])
    va[...] = band_seg(sy[0], 0)
    vb[...] = band_seg(sy[1], 0)


def group_of(j):
    g = (j >= 3).astype(jnp.int32) + (j >= 6) + (j >= 9) + (j >= 12)
    return g, j - 3 * g


def pack_kernel(foot, tail, xa, xb, va, vb):
    _, _, sy, sx = sides()
    j = iota((16, 160), 0)
    kk = iota((16, 160), 1)
    g, s = group_of(j)
    same = ((kk >> 5) == g) & (j < 15)
    comp = (kk & 31) - s

    def pick(d):
        return hot(same & (comp == 3 * d))

    last = tail[...]
    send_all(pick, foot.at[0:32, :], last, last, (xa, xb, va, vb), sy, sx)


def slot_masks(table, total):
    own = table[:, 0:1]
    idx = NBR * table[:, 1:2] + table[:, 2:3]
    live = iota((MP, 1), 0) < total
    return own, idx, live


def slot_select(table, total):
    ids, idx, live = slot_masks(table, total)
    j5 = iota((5 * MP, 16), 1)
    g5 = iota((5 * MP, 16), 0) >> 4
    s5 = j5 - 3 * g5
    idx5 = jnp.concatenate([jnp.where(live, idx, -100)] * 5, axis=0)
    fits = (s5 >= 0) & (s5 < 3)

    def select(d):
        return hot(fits & (idx5 == 3 * d + s5))

    return ids, live, select


NT = (((1,), (1,)), ((), ()))


def own_kernel(count, res, foot, tr, table, rest, first, own, ctr):
    ids, _, _ = slot_masks(table, count[...])
    own_hot = hot(ids == iota((MP, K), 1))
    c_own = dot(own_hot, tr[...])
    ctr[...] = c_own
    eye = hot(iota((CH, CH), 0) == iota((CH, CH), 1))
    both = jnp.concatenate([c_own.astype(bf16), eye], axis=0)
    width = 512
    for n in range(NPIX // width):
        lanes = slice(width * n, width * (n + 1))
        own[:, lanes] = dot(own_hot, foot[:, lanes])
        turned = lax.dot_general(both, res[lanes, :], NT, preferred_element_type=f32)
        first[:, lanes] = turned[0:MP]
        rest[:, lanes] = turned[MP:].astype(bf16)


def side_kernel(rows, cols, row_ref, col_ref, count, table, rxa, rxb, side, crem):
    row, col, _, sx = sides()
    _, _, select = slot_select(table, count[...])
    whole, tail = receive_sides(
        select, MP, (rxa, rxb), row, col, sx, row_ref, col_ref, rows, cols
    )
    crem[...] = tail[:, 0:F]
    for m in range(32):
        side[:, CH * m : CH * (m + 1)] = whole[MP * m : MP * (m + 1)]


def refit_kernel(
    rows, cols, row_in, col_in, count, res, rest, first, own, ctr, side, crem, table, wide, rya, ryb,
    xa, xb, va, vb, merged, mtrace, acc, pbuf, row_ref, col_ref, sem,
):
    ready = fetch(row_in, col_in, row_ref, col_ref, sem)
    row, col, sy, sx = sides()
    total = count[...]
    _, live, select = slot_select(table, total)
    acc[...] = side[...]
    c_own = ctr[...]
    c_rem = crem[...]
    bands = receive_bands(
        (select, select), MP, (rya, ryb), pbuf, row, col, sy, sx, row_ref, col_ref, rows, cols, ready
    )
    for u, (moved, tail) in enumerate(bands):
        c_rem = c_rem + tail[:, 0:F]
        start = band_start(sy[u])
        for m in range(12):
            lanes = pl.ds(pl.multiple_of(start + CH * m, CH), CH)
            acc[:, lanes] += moved[MP * m : MP * (m + 1)]
    trace = c_own
    step = 512
    for it in range(ITERS):
        tb = trace.astype(bf16)
        co = jnp.sum(c_own * trace, axis=1, keepdims=True)
        cr = jnp.sum(c_rem * trace, axis=1, keepdims=True)
        scale = 1.0 / (jnp.sum(trace * trace, axis=1, keepdims=True) + epsilon * F)
        lanes = [slice(step * n, step * (n + 1)) for n in range(NPIX // step)]
        if it == 0:
            across = [first[:, cut] for cut in lanes]
        else:
            across = [dot(tb, rest[:, cut]) for cut in lanes]
        sa = jnp.zeros((MP, CH), f32)
        sr = jnp.zeros((MP, CH), f32)
        ss = jnp.zeros((MP, CH), f32)
        shapes = []
        for n, cut in enumerate(lanes):
            ao = own[:, cut]
            ar = acc[:, cut]
            now = jnp.maximum(across[n] + ao * co + ar * cr, 0.0) * scale
            shapes.append(now.astype(bf16))
            if it == ITERS - 1:
                merged[:, cut] = jnp.where(live, now, 0.0).astype(bf16)
            pa = ao * now
            pr = ar * now
            ps = now * now
            for q in range(step // CH):
                part = slice(CH * q, CH * (q + 1))
                sa = sa + pa[:, part]
                sr = sr + pr[:, part]
                ss = ss + ps[:, part]
        down = sum(dot(shapes[n], res[cut, :]) for n, cut in enumerate(lanes))
        down = (
            down
            + c_own * jnp.sum(sa, axis=1, keepdims=True)
            + c_rem * jnp.sum(sr, axis=1, keepdims=True)
        )
        trace = jnp.maximum(down, 0.0) / (jnp.sum(ss, axis=1, keepdims=True) + epsilon * NPIX)
    tout = jnp.where(live, trace, 0.0).astype(bf16)
    mtrace[...] = tout
    j = iota((16, 5 * MP), 0)
    kk = iota((16, 5 * MP), 1)
    g, s = group_of(j)
    slot = kk & 15
    same = ((kk >> 4) == g) & (j < 15) & (slot < total)
    comp = NBR * wide[1:2, :] + wide[2:3, :] - s

    def pick(d):
        return hot(same & (comp == 3 * d))

    ones = jnp.ones((MP, CH), bf16)
    blank = jnp.zeros((MP, CH), bf16)
    tail = jnp.concatenate([tout, ones, blank], axis=1)
    send_all(pick, merged, tail, tail, (xa, xb, va, vb), sy, sx)


def corr_kernel(comp, tr, rxa, rxb, rya, ryb, out):
    _, _, sy, sx = sides()
    k = iota((BORDER, 16), 0)
    j = iota((BORDER, 16), 1)
    s = j - 12
    fits = (s >= 0) & (s < 3)
    z = jnp.zeros((BORDER, F), f32)
    for t, ref in enumerate((rxa, rxb)):
        at = 2 * CW + 512
        z = z + dot(hot(fits & (k == 3 * direction(0, sx[t]) + s)), ref[:, at : at + F])
    for u, ref in enumerate((rya, ryb)):
        for q, dx in enumerate((0, sx[0], sx[1])):
            z = z + dot(hot(fits & (k == 3 * direction(sy[u], dx) + s)), ref[:, CW * q : CW * q + F])
    x = tr[...].astype(f32)
    x = x - jnp.mean(x, axis=1, keepdims=True)
    z = z - jnp.mean(z, axis=1, keepdims=True)
    high = lax.Precision.HIGHEST
    cov = lax.dot_general(z, x, NT, precision=high, preferred_element_type=f32) / F
    vz = jnp.mean(z * z, axis=1, keepdims=True)
    ones = jnp.ones((8, F), f32)
    vx = lax.dot_general(ones, x * x, NT, precision=high, preferred_element_type=f32)[0:1] / F
    alive = iota((1, K), 1) < comp[...]
    out[...] = jnp.where(alive, cov / jnp.sqrt((vx + epsilon) * (vz + epsilon)), 0.0)


def row_select(n, first):
    j5 = iota((5 * n, 16), 1)
    r5 = iota((5 * n, 16), 0)
    s5 = j5 - 3 * (r5 >> 4)
    k5 = (r5 & 15) + first
    fits = (s5 >= 0) & (s5 < 3)

    def select(d):
        return hot(fits & (k5 == 3 * d + s5))

    return select


def before_kernel(
    rows, cols, row_ref, col_ref, count, compc, foot, tr, wide, merged, mtrace, rxa, rxb,
    base, tbase, upper, lower,
):
    row, col, _, sx = sides()
    n = 16
    whole, tail = receive_sides(
        row_select(n, 8), n, (rxa, rxb), row, col, sx, row_ref, col_ref, rows, cols
    )
    flag = tail[:, CH : CH + 1] > 0.5
    k = iota((n, 1), 0) + 8
    _, _, _, c_lf = pixel_shift(0, -1, row, col, row_ref, col_ref, rows, cols)
    _, _, _, c_rt = pixel_shift(0, 1, row, col, row_ref, col_ref, rows, cols)
    x_lo = jnp.where(k >= 12, PW - c_rt, 0)
    x_hi = jnp.where(flag, jnp.where(k < 12, c_lf, PW), 0)
    x = iota((1, CH), 1) & (PW - 1)
    inside = (x >= x_lo) & (x < x_hi)
    total = count[...]
    own_id = wide[0:1, 0:MP]
    own_mask = (iota((K - BORDER, MP), 0) + BORDER == own_id) & (iota((K - BORDER, MP), 1) < total)
    own_hot = hot(own_mask)
    hit = jnp.sum(own_hot.astype(f32), axis=1, keepdims=True) > 0.5
    alive = iota((K - BORDER, 1), 0) + BORDER < compc[...]
    step = 512
    for b in range(NPIX // step):
        lanes = slice(step * b, step * (b + 1))
        mine = foot[:, lanes].astype(f32)
        got = dot(own_hot, merged[:, lanes])
        low = jnp.where(alive, jnp.where(hit, got, mine[BORDER:]), 0.0)
        mid = []
        for q in range(step // CH):
            m = b * (step // CH) + q
            mid.append(
                jnp.where(
                    inside, whole[n * m : n * (m + 1)], mine[8:BORDER, CH * q : CH * (q + 1)]
                )
            )
        mid = jnp.concatenate(mid, axis=1)
        base[:, lanes] = jnp.concatenate([mine[0:8], mid, low], axis=0).astype(bf16)
        if step * b < BAND:
            upper[:, lanes] = jnp.concatenate([mine[0:8], mid[0:8]], axis=0)
        if step * b >= LOW:
            lower[:, step * b - LOW : step * (b + 1) - LOW] = mid
    mine = tr[...].astype(f32)
    mid = jnp.where(flag, tail[:, 0:F], mine[8:BORDER])
    low = jnp.where(alive, jnp.where(hit, dot(own_hot, mtrace[...]), mine[BORDER:]), 0.0)
    tbase[...] = jnp.concatenate([mine[0:8], mid, low], axis=0)


def final_kernel(
    rows, cols, row_in, col_in, base, tbase, upper, lower, rya, ryb,
    nfoot, ntrace, placed, tails, pbuf, out, row_ref, col_ref, sem,
):
    ready = fetch(row_in, col_in, row_ref, col_ref, sem)
    row, col, sy, sx = sides()
    n = 16
    downs = [jnp.where(sy[u] > 0, 1, 0) for u in range(2)]
    bands = receive_bands(
        [row_select(n, 8 * dn) for dn in downs],
        n, (rya, ryb), pbuf, row, col, sy, sx, row_ref, col_ref, rows, cols, ready,
    )
    for dn, (moved, tail) in zip(downs, bands):
        for m in range(12):
            placed[dn, :, CH * m : CH * (m + 1)] = moved[n * m : n * (m + 1)]
        tails[dn] = tail
    _, _, r_up, _ = pixel_shift(-1, 0, row, col, row_ref, col_ref, rows, cols)
    _, _, r_dn, _ = pixel_shift(1, 0, row, col, row_ref, col_ref, rows, cols)
    _, _, _, c_lf = pixel_shift(0, -1, row, col, row_ref, col_ref, rows, cols)
    _, _, _, c_rt = pixel_shift(0, 1, row, col, row_ref, col_ref, rows, cols)
    k = iota((n, 1), 0)
    pix = iota((1, BAND), 1)
    y = pix >> 6
    x = pix & (PW - 1)
    copies = []
    for dn, edge in enumerate((upper, lower)):
        j = k - 7 * dn
        flag = tails[dn, :, CH : CH + 1] > 0.5
        x_lo = jnp.where(j >= 6, PW - c_rt, 0)
        x_hi = jnp.where(flag, jnp.where(j < 3, c_lf, PW), 0)
        y_ok = (y < r_up) if dn == 0 else (y >= OV_HI - r_dn)
        inside = y_ok & (x >= x_lo) & (x < x_hi)
        out[dn] = jnp.where(inside, placed[dn], edge[...]).astype(bf16)
        copies.append(
            pltpu.make_async_copy(
                out.at[dn],
                nfoot.at[8 * dn : 8 * dn + 16, LOW * dn : LOW * dn + BAND],
                sem.at[2 + dn],
            )
        )
        copies[-1].start()
    mine = tbase[0:BORDER]
    gap = jnp.zeros((8, 2 * CH), f32)
    both = jnp.concatenate([tails[0], gap], axis=0) + jnp.concatenate([gap, tails[1]], axis=0)
    top = jnp.where(both[:, CH : CH + 1] > 0.5, both[:, 0:F], mine)
    ntrace[...] = jnp.concatenate([top, tbase[BORDER:]], axis=0).astype(bf16)
    for copy in copies:
        copy.wait()


SMEM = pl.BlockSpec(memory_space=pltpu.SMEM)
VMEM = pl.BlockSpec(memory_space=pltpu.VMEM)
LIMIT = 24 * 1024 * 1024


def shape(*dims, dtype=bf16):
    return jax.ShapeDtypeStruct(dims, dtype)


PACKETS = (shape(16, XW), shape(16, XW), shape(16, CW), shape(16, CW))
HBM = pl.BlockSpec(memory_space=pltpu.HBM)


def call(kernel, outs, ins, out_specs, scratch, flops, aliases={}):
    return pl.pallas_call(
        kernel,
        out_shape=outs,
        in_specs=ins,
        out_specs=out_specs,
        scratch_shapes=scratch,
        input_output_aliases=aliases,
        compiler_params=pltpu.CompilerParams(vmem_limit_bytes=LIMIT),
        cost_estimate=pl.CostEstimate(flops=flops, bytes_accessed=1 << 20, transcendentals=0),
    )


def swap(value, axis, parity):
    count = lax.axis_size(axis)
    pairs = []
    for i in range(parity, count - 1, 2):
        pairs += [(i, i + 1), (i + 1, i)]
    return lax.ppermute(value, axis, pairs)


def exchange(xa, xb, va, vb):
    rxb = swap(xb, "px", 1)
    rxa = swap(xa, "px", 0)
    yb = jnp.concatenate([vb, rxa[:, CW : 2 * CW], rxb[:, CW : 2 * CW]], axis=1)
    ya = jnp.concatenate([va, rxa[:, 0:CW], rxb[:, 0:CW]], axis=1)
    ryb = swap(yb, "py", 1)
    rya = swap(ya, "py", 0)
    return rxa, rxb, rya, ryb


def body(
    residual, footprints, traces, merge_pairs, pair_counts, comp_counts, row_inter, col_inter
):
    res = residual[0, 0]
    foot = footprints[0, 0]
    tr = traces[0, 0]
    table = merge_pairs[0, 0]
    wide = jnp.tile(table.T, (1, 5))
    rows, cols = lax.axis_size("py"), lax.axis_size("px")

    def geo(kernel):
        def run(*refs):
            kernel(rows, cols, *refs)

        return run

    packets = call(
        pack_kernel, PACKETS, [VMEM] * 2, (VMEM,) * 4, [], 1 << 24
    )(foot, jnp.pad(tr[:32], ((0, 0), (0, 2 * CH))))
    rxa, rxb, rya, ryb = exchange(*packets)

    prepared = call(
        own_kernel,
        (
            shape(F, NPIX),
            shape(MP, NPIX, dtype=f32),
            shape(MP, NPIX, dtype=f32),
            shape(MP, F, dtype=f32),
        ),
        [VMEM] * 5,
        (VMEM,) * 4,
        [],
        1 << 24,
    )(pair_counts, res, foot, tr, table)

    placed = call(
        geo(side_kernel),
        (shape(MP, NPIX, dtype=f32), shape(MP, F, dtype=f32)),
        [SMEM] * 2 + [VMEM] * 4,
        (VMEM,) * 2,
        [],
        1 << 24,
    )(row_inter, col_inter, pair_counts, table, rxa, rxb)

    xa, xb, va, vb, merged, mtrace = call(
        geo(refit_kernel),
        PACKETS + (shape(MP, NPIX), shape(MP, F)),
        [VMEM] * 14,
        (VMEM,) * 6,
        [
            pltpu.VMEM((MP, NPIX), f32),
            pltpu.VMEM((6, MP, PBW), bf16),
            pltpu.SMEM((rows - 1,), jnp.int32),
            pltpu.SMEM((cols - 1,), jnp.int32),
            pltpu.SemaphoreType.DMA((2,)),
        ],
        1 << 28,
    )(row_inter, col_inter, pair_counts, res, *prepared, *placed, table, wide, rya, ryb)
    back = exchange(xa, xb, va, vb)

    corr = call(
        corr_kernel, shape(BORDER, K, dtype=f32), [VMEM] * 6, VMEM, [], 1 << 22
    )(comp_counts, tr, rxa, rxb, rya, ryb)

    partial = call(
        geo(before_kernel),
        (
            shape(K, NPIX),
            shape(K, F, dtype=f32),
            shape(16, BAND, dtype=f32),
            shape(16, BAND, dtype=f32),
        ),
        [SMEM] * 2 + [VMEM] * 9,
        (VMEM,) * 4,
        [],
        1 << 24,
    )(row_inter, col_inter, pair_counts, comp_counts, foot, tr, wide, merged, mtrace, *back[:2])

    nfoot, ntrace = call(
        geo(final_kernel),
        (shape(K, NPIX), shape(K, F)),
        [VMEM] * 2 + [HBM] + [VMEM] * 5,
        (HBM, VMEM),
        [
            pltpu.VMEM((2, 16, BAND), f32),
            pltpu.VMEM((2, 16, 2 * CH), f32),
            pltpu.VMEM((6, 16, PBW), bf16),
            pltpu.VMEM((2, 16, BAND), bf16),
            pltpu.SMEM((rows - 1,), jnp.int32),
            pltpu.SMEM((cols - 1,), jnp.int32),
            pltpu.SemaphoreType.DMA((4,)),
        ],
        1 << 26,
        {2: 0},
    )(row_inter, col_inter, *partial, *back[2:])
    return nfoot[None, None], ntrace[None, None], corr.T[None, None]


def solution(mesh):
    in_specs = (
        P("py", "px", None, None),
        P("py", "px", None, None),
        P("py", "px", None, None),
        P("py", "px", None, None),
        P("py", "px"),
        P("py", "px"),
        P(),
        P(),
    )
    out_specs = (P("py", "px", None, None), P("py", "px", None, None), P("py", "px", None, None))
    return jax.shard_map(body, mesh=mesh, in_specs=in_specs, out_specs=out_specs, check_vma=False)
```

```python
import jax
import jax.numpy as jnp
from jax import lax
from jax.experimental import pallas as pl
from jax.experimental.pallas import tpu as pltpu
from jax.sharding import PartitionSpec as P


PH = 64
PW = 64
NPIX = PH * PW
K = 40
NBR = 3
BORDER = 24
MP = 16
F = 128
ITERS = 4
OV_HI = 24
epsilon = 1e-05

BAND = OV_HI * PW
LOW = NPIX - BAND
CW = BAND // 4
EW = 896
XW = 2 * CW + EW
CH = 128
PAD = 9
PBW = (PAD + 12 + PAD) * CH

f32 = jnp.float32
bf16 = jnp.bfloat16


def iota(shape, dim):
    return lax.broadcasted_iota(jnp.int32, shape, dim)


def sides():
    row = lax.axis_index("py")
    col = lax.axis_index("px")
    sy = 1 - 2 * lax.rem(row, 2)
    sx = 1 - 2 * lax.rem(col, 2)
    return row, col, (sy, -sy), (sx, -sx)


def direction(dy, dx):
    flat = (dy + 1) * 3 + dx + 1
    return flat - (flat > 4).astype(jnp.int32) if not isinstance(flat, int) else flat - (flat > 4)


def hot(mask):
    return jnp.where(mask, 1.0, 0.0).astype(bf16)


def dot(a, b):
    return jnp.dot(a, b, preferred_element_type=f32)


def band_start(dy):
    return jnp.where(dy > 0, LOW, 0)


def pack_rows(pick, pieces, tail):
    return dot(pick, jnp.concatenate(pieces + [tail], axis=0)).astype(bf16)


def pixel_shift(dy, dx, geo):
    ri = jnp.where(dy > 0, geo[0, 1], geo[0, 0])
    ci = jnp.where(dx > 0, geo[0, 3], geo[0, 2])
    return dy * (OV_HI - ri), dx * (PW - ci)


def column_matrix(ox):
    i = iota((CH, CH), 0)
    o = iota((CH, CH), 1)
    x = (o & (PW - 1)) - ox
    return hot((i == o - ox) & (x >= 0) & (x < PW))


def band_matrix(odd, ox):
    i = iota((2 * CH, CH), 0)
    o = iota((2 * CH, CH), 1)
    x = (o & (PW - 1)) - ox
    return hot((i == o + CH - PW * odd - ox) & (x >= 0) & (x < PW))


def place_whole(whole, ox):
    stack = jnp.concatenate(
        [whole[:, CH * m : CH * (m + 1)] for m in range(32)], axis=0
    ).astype(bf16)
    return dot(stack, column_matrix(ox))


def receive_sides(select, n, xs, sx, geo, ready):
    tail = jnp.zeros((n, 2 * CH), f32)
    whole = None
    taken = [dot(select(direction(0, sx[t])), xs[t][:, 2 * CW : XW]) for t in range(2)]
    ready()
    for t, picked in enumerate(taken):
        full = jnp.concatenate(
            [picked[n * g : n * (g + 1)] for g in range(4)] + [picked[4 * n :, 0:512]], axis=1
        )
        tail = tail + picked[4 * n :, 512 : 512 + 2 * CH]
        _, ox = pixel_shift(0, sx[t], geo)
        moved = place_whole(full, ox)
        whole = moved if whole is None else whole + moved
    return whole, tail


def clear_pads(pbuf):
    pbuf[:, :, 0 : PAD * CH] = jnp.zeros(pbuf.shape[:2] + (PAD * CH,), bf16)
    pbuf[:, :, PAD * CH + BAND :] = jnp.zeros(pbuf.shape[:2] + (PBW - PAD * CH - BAND,), bf16)


def receive_bands(selects, n, ys, pbuf, sy, sx, geo, ready):
    steps = (0, sx[0], sx[1])
    picked = [
        [
            dot(selects[u](direction(sy[u], dx)), ys[u][:, CW * j : CW * (j + 1)])
            for j, dx in enumerate(steps)
        ]
        for u in range(2)
    ]
    clear_pads(pbuf)
    ready()
    for u in range(2):
        for j in range(3):
            for g in range(4):
                at = PAD * CH + CW * g
                pbuf[3 * u + j, :, at : at + CW] = picked[u][j][n * g : n * (g + 1)].astype(bf16)
    out = []
    for u in range(2):
        moved = None
        tail = jnp.zeros((n, 2 * CH), f32)
        for j, dx in enumerate(steps):
            shift, ox = pixel_shift(sy[u], dx, geo)
            first = (PAD - 1 - (shift >> 1)) * CH
            stack = jnp.concatenate(
                [
                    pbuf[3 * u + j, :, pl.ds(pl.multiple_of(first + CH * m, CH), 2 * CH)]
                    for m in range(12)
                ],
                axis=0,
            )
            one = dot(stack, band_matrix(shift & 1, ox))
            moved = one if moved is None else moved + one
            tail = tail + picked[u][j][4 * n :, 0 : 2 * CH]
        out.append((moved, tail))
    return out


def begin(*copies):
    loads = [pltpu.make_async_copy(*copy) for copy in copies]
    for load in loads:
        load.start()

    def ready():
        for load in loads:
            load.wait()

    return ready


def send_all(pick, src, tail_narrow, tail_wide, outs, sy, sx):
    xa, xb, va, vb = outs

    def band_seg(dy, dx):
        start = band_start(dy)
        pieces = [
            src[:, pl.ds(pl.multiple_of(start + CW * g, CH), CW)] for g in range(4)
        ]
        return pack_rows(pick(direction(dy, dx)), pieces, tail_narrow)

    def whole_seg(dx):
        pieces = [src[:, EW * g : EW * (g + 1)] for g in range(4)]
        last = jnp.concatenate([src[:, 4 * EW : NPIX], tail_wide], axis=1)
        return pack_rows(pick(direction(0, dx)), pieces, last)

    for t, out in enumerate((xa, xb)):
        out[:, 0:CW] = band_seg(sy[0], sx[t])
        out[:, CW : 2 * CW] = band_seg(sy[1], sx[t])
        out[:, 2 * CW : XW] = whole_seg(sx[t])
    va[...] = band_seg(sy[0], 0)
    vb[...] = band_seg(sy[1], 0)


def group_of(j):
    g = (j >= 3).astype(jnp.int32) + (j >= 6) + (j >= 9) + (j >= 12)
    return g, j - 3 * g


def pack_kernel(foot, tr, xa, xb, va, vb, src, trs, sem):
    ready = begin(
        (foot.at[0:32, :], src, sem.at[0]), (tr.at[0:32, :], trs, sem.at[1])
    )
    _, _, sy, sx = sides()
    j = iota((16, 160), 0)
    kk = iota((16, 160), 1)
    g, s = group_of(j)
    same = ((kk >> 5) == g) & (j < 15)
    comp = (kk & 31) - s

    def pick(d):
        return hot(same & (comp == 3 * d))

    ready()
    tail = jnp.concatenate([trs[...], jnp.zeros((32, 2 * CH), bf16)], axis=1)
    send_all(pick, src, tail, tail, (xa, xb, va, vb), sy, sx)


def slot_select(table):
    j5 = iota((5 * MP, 16), 1)
    g5 = iota((5 * MP, 16), 0) >> 4
    s5 = j5 - 3 * g5
    idx5 = jnp.concatenate([table[:, 1:2]] * 5, axis=0)
    fits = (s5 >= 0) & (s5 < 3)

    def select(d):
        return hot(fits & (idx5 == 3 * d + s5))

    return select


NT = (((1,), (1,)), ((), ()))


HALF = NPIX // 2


def load_half(res_in, start, res, sem):
    width = 512
    return [
        begin(
            (
                res_in.at[start + width * n : start + width * (n + 1), :],
                res.at[width * n : width * (n + 1), :],
                sem.at[n],
            )
        )
        for n in range(HALF // width)
    ]


def turn_half(loads, c_own, res, rest, first):
    width = 512
    eye = hot(iota((CH, CH), 0) == iota((CH, CH), 1))
    both = jnp.concatenate([c_own.astype(bf16), eye], axis=0)
    for n, load in enumerate(loads):
        lanes = slice(width * n, width * (n + 1))
        load()
        turned = lax.dot_general(both, res[lanes, :], NT, preferred_element_type=f32)
        first[:, lanes] = turned[0:MP]
        rest[:, lanes] = turned[MP:].astype(bf16)


def own_kernel(
    rows, cols, count, row_in, col_in, res_in, tr_in, table, wide,
    res, rest, first, ctr, slots, across, geo, tr, row_ref, col_ref, sem, rsem,
):
    small = begin((tr_in, tr, sem.at[0]))
    loads = load_half(res_in, 0, res, rsem)
    scalars = begin((row_in, row_ref, sem.at[1]), (col_in, col_ref, sem.at[2]))
    row, col, _, _ = sides()
    total = count[0, 0]
    ids = table[:, 0:1]
    live = iota((MP, CH), 0) < total
    idx = NBR * table[:, 1:2] + table[:, 2:3]
    place = iota((MP, CH), 1)
    dead = jnp.where(live, jnp.where(place == 0, ids, idx), -100)
    slots[...] = jnp.where(place == 2, ids, dead)
    line = iota((8, CH), 0)
    alive = (iota((8, CH), 1) & 15) < total
    pair = NBR * wide[1:2, :] + wide[2:3, :]
    across[...] = jnp.where(alive, jnp.where(line == 0, wide[0:1, :], pair), -100)
    own_hot = hot(ids == iota((MP, K), 1))
    small()
    c_own = dot(own_hot, tr[...])
    ctr[...] = c_own
    turn_half(loads, c_own, res, rest, first)
    scalars()
    up = row_ref[jnp.clip(row - 1, 0, rows - 2)]
    down = row_ref[jnp.clip(row, 0, rows - 2)]
    left = col_ref[jnp.clip(col - 1, 0, cols - 2)]
    right = col_ref[jnp.clip(col, 0, cols - 2)]
    lane = iota((1, CH), 1)
    geo[...] = jnp.where(
        lane == 0, up, jnp.where(lane == 1, down, jnp.where(lane == 2, left, right))
    )


def side_kernel(
    res_in, foot_in, geo_in, ctr, slots, rxa, rxb, res, rest, first, own, side, crem, foot, geo, sem, rsem
):
    loads = load_half(res_in, HALF, res, rsem)
    load = begin((foot_in, foot, sem.at[1]))
    ready = begin((geo_in, geo, sem.at[0]))
    _, _, _, sx = sides()
    own_hot = hot(slots[:, 2:3] == iota((MP, K), 1))
    whole, tail = receive_sides(slot_select(slots), MP, (rxa, rxb), sx, geo, ready)
    crem[...] = tail[:, 0:F]
    for m in range(32):
        side[:, CH * m : CH * (m + 1)] = whole[MP * m : MP * (m + 1)]
    turn_half(loads, ctr[...], res, rest, first)
    load()
    own[...] = dot(own_hot, foot[...])


def refit_kernel(
    geo_in, res_l, rest_l, first_l, ctr, slots, wide, res_h, rest_h, first_h, own, side, crem, rya, ryb,
    xa, xb, va, vb, merged, mtrace, acc, pbuf, geo, sem,
):
    ready = begin((geo_in, geo, sem.at[0]))
    _, _, sy, sx = sides()
    live = slots[:, 1:2] >= 0
    select = slot_select(slots)
    acc[...] = side[...]
    c_own = ctr[...]
    c_rem = crem[...]
    bands = receive_bands((select, select), MP, (rya, ryb), pbuf, sy, sx, geo, ready)
    for u, (moved, tail) in enumerate(bands):
        c_rem = c_rem + tail[:, 0:F]
        start = band_start(sy[u])
        for m in range(12):
            lanes = pl.ds(pl.multiple_of(start + CH * m, CH), CH)
            acc[:, lanes] += moved[MP * m : MP * (m + 1)]
    trace = c_own
    step = 512
    for it in range(ITERS):
        tb = trace.astype(bf16)
        co = jnp.sum(c_own * trace, axis=1, keepdims=True)
        cr = jnp.sum(c_rem * trace, axis=1, keepdims=True)
        scale = 1.0 / (jnp.sum(trace * trace, axis=1, keepdims=True) + epsilon * F)
        lanes = [slice(step * n, step * (n + 1)) for n in range(NPIX // step)]
        halves = [slice(step * n, step * (n + 1)) for n in range(HALF // step)]
        if it == 0:
            across = [f[:, cut] for f in (first_l, first_h) for cut in halves]
        else:
            across = [dot(tb, r[:, cut]) for r in (rest_l, rest_h) for cut in halves]
        sa = jnp.zeros((MP, CH), f32)
        sr = jnp.zeros((MP, CH), f32)
        ss = jnp.zeros((MP, CH), f32)
        shapes = []
        for n, cut in enumerate(lanes):
            ao = own[:, cut]
            ar = acc[:, cut]
            now = jnp.maximum(across[n] + ao * co + ar * cr, 0.0) * scale
            shapes.append(now.astype(bf16))
            if it == ITERS - 1:
                merged[:, cut] = jnp.where(live, now, 0.0).astype(bf16)
            pa = ao * now
            pr = ar * now
            ps = now * now
            for q in range(step // CH):
                part = slice(CH * q, CH * (q + 1))
                sa = sa + pa[:, part]
                sr = sr + pr[:, part]
                ss = ss + ps[:, part]
        parts = [r[cut, :] for r in (res_l, res_h) for cut in halves]
        down = sum(dot(now, part) for now, part in zip(shapes, parts))
        down = (
            down
            + c_own * jnp.sum(sa, axis=1, keepdims=True)
            + c_rem * jnp.sum(sr, axis=1, keepdims=True)
        )
        trace = jnp.maximum(down, 0.0) / (jnp.sum(ss, axis=1, keepdims=True) + epsilon * NPIX)
    tout = jnp.where(live, trace, 0.0).astype(bf16)
    mtrace[...] = tout
    j = iota((16, 5 * MP), 0)
    kk = iota((16, 5 * MP), 1)
    g, s = group_of(j)
    same = ((kk >> 4) == g) & (j < 15)
    comp = wide[1:2, 0 : 5 * MP] - s

    def pick(d):
        return hot(same & (comp == 3 * d))

    ones = jnp.ones((MP, CH), bf16)
    blank = jnp.zeros((MP, CH), bf16)
    tail = jnp.concatenate([tout, ones, blank], axis=1)
    send_all(pick, merged, tail, tail, (xa, xb, va, vb), sy, sx)


def correlate(alive, tr, rxa, rxb, rya, ryb, out, sy, sx):
    k = iota((BORDER, 16), 0)
    j = iota((BORDER, 16), 1)
    s = j - 12
    fits = (s >= 0) & (s < 3)
    z = jnp.zeros((BORDER, F), f32)
    for t, ref in enumerate((rxa, rxb)):
        at = 2 * CW + 512
        z = z + dot(hot(fits & (k == 3 * direction(0, sx[t]) + s)), ref[:, at : at + F])
    for u, ref in enumerate((rya, ryb)):
        for q, dx in enumerate((0, sx[0], sx[1])):
            z = z + dot(hot(fits & (k == 3 * direction(sy[u], dx) + s)), ref[:, CW * q : CW * q + F])
    x = tr.astype(f32)
    x = x - jnp.mean(x, axis=1, keepdims=True)
    z = z - jnp.mean(z, axis=1, keepdims=True)
    high = lax.Precision.HIGHEST
    cov = lax.dot_general(z, x, NT, precision=high, preferred_element_type=f32) / F
    vz = jnp.mean(z * z, axis=1, keepdims=True)
    ones = jnp.ones((8, F), f32)
    vx = lax.dot_general(ones, x * x, NT, precision=high, preferred_element_type=f32)[0:1] / F
    out[...] = jnp.where(alive, cov / jnp.sqrt((vx + epsilon) * (vz + epsilon)), 0.0)


def row_select(n, first):
    j5 = iota((5 * n, 16), 1)
    r5 = iota((5 * n, 16), 0)
    s5 = j5 - 3 * (r5 >> 4)
    k5 = (r5 & 15) + first
    fits = (s5 >= 0) & (s5 < 3)

    def select(d):
        return hot(fits & (k5 == 3 * d + s5))

    return select


def before_kernel(
    comp, foot_in, tr_in, geo_in, wide, merged, mtrace, oxa, oxb, oya, oyb, rxa, rxb,
    base, tbase, upper, lower, corr, foot, tr, geo, sem,
):
    quick = begin((geo_in, geo, sem.at[0]))
    ready = begin((tr_in, tr, sem.at[1]), (foot_in, foot, sem.at[2]))
    _, _, sy, sx = sides()
    n = 16
    whole, tail = receive_sides(row_select(n, 8), n, (rxa, rxb), sx, geo, quick)
    flag = tail[:, CH : CH + 1] > 0.5
    k = iota((n, 1), 0) + 8
    x_lo = jnp.where(k >= 12, PW - geo[0, 3], 0)
    x_hi = jnp.where(flag, jnp.where(k < 12, geo[0, 2], PW), 0)
    x = iota((1, CH), 1) & (PW - 1)
    inside = (x >= x_lo) & (x < x_hi)
    own_hot = hot(iota((K - BORDER, MP), 0) + BORDER == wide[0:1, 0:MP])
    hit = jnp.sum(own_hot.astype(f32), axis=1, keepdims=True) > 0.5
    ready()
    correlate(iota((1, K), 1) < comp[0, 0], tr[...], oxa, oxb, oya, oyb, corr, sy, sx)
    alive = iota((K - BORDER, 1), 0) + BORDER < comp[0, 0]
    step = 512
    for b in range(NPIX // step):
        lanes = slice(step * b, step * (b + 1))
        mine = foot[:, lanes].astype(f32)
        got = dot(own_hot, merged[:, lanes])
        low = jnp.where(alive, jnp.where(hit, got, mine[BORDER:]), 0.0)
        mid = []
        for q in range(step // CH):
            m = b * (step // CH) + q
            mid.append(
                jnp.where(
                    inside, whole[n * m : n * (m + 1)], mine[8:BORDER, CH * q : CH * (q + 1)]
                )
            )
        mid = jnp.concatenate(mid, axis=1)
        base[:, lanes] = jnp.concatenate([mine[0:8], mid, low], axis=0).astype(bf16)
        if step * b < BAND:
            upper[:, lanes] = jnp.concatenate([mine[0:8], mid[0:8]], axis=0)
        if step * b >= LOW:
            lower[:, step * b - LOW : step * (b + 1) - LOW] = mid
    mine = tr[...].astype(f32)
    mid = jnp.where(flag, tail[:, 0:F], mine[8:BORDER])
    low = jnp.where(alive, jnp.where(hit, dot(own_hot, mtrace[...]), mine[BORDER:]), 0.0)
    tbase[...] = jnp.concatenate([mine[0:8], mid, low], axis=0)


def final_kernel(
    geo_in, base, tbase, upper, lower, rya, ryb,
    nfoot, ntrace, placed, tails, pbuf, out, tout, geo, sem,
):
    ready = begin((geo_in, geo, sem.at[0]))
    _, _, sy, sx = sides()
    n = 16
    downs = [jnp.where(sy[u] > 0, 1, 0) for u in range(2)]
    bands = receive_bands(
        [row_select(n, 8 * dn) for dn in downs], n, (rya, ryb), pbuf, sy, sx, geo, ready
    )
    for dn, (moved, tail) in zip(downs, bands):
        for m in range(12):
            placed[dn, :, CH * m : CH * (m + 1)] = moved[n * m : n * (m + 1)]
        tails[dn] = tail
    mine = tbase[0:BORDER]
    gap = jnp.zeros((8, 2 * CH), f32)
    both = jnp.concatenate([tails[0], gap], axis=0) + jnp.concatenate([gap, tails[1]], axis=0)
    top = jnp.where(both[:, CH : CH + 1] > 0.5, both[:, 0:F], mine)
    tout[...] = jnp.concatenate([top, tbase[BORDER:]], axis=0).astype(bf16)
    copies = [pltpu.make_async_copy(tout, ntrace, sem.at[1])]
    copies[0].start()
    r_up, r_dn, c_lf, c_rt = (geo[0, i] for i in range(4))
    k = iota((n, 1), 0)
    pix = iota((1, BAND), 1)
    y = pix >> 6
    x = pix & (PW - 1)
    for dn, edge in enumerate((upper, lower)):
        j = k - 7 * dn
        flag = tails[dn, :, CH : CH + 1] > 0.5
        x_lo = jnp.where(j >= 6, PW - c_rt, 0)
        x_hi = jnp.where(flag, jnp.where(j < 3, c_lf, PW), 0)
        y_ok = (y < r_up) if dn == 0 else (y >= OV_HI - r_dn)
        inside = y_ok & (x >= x_lo) & (x < x_hi)
        out[dn] = jnp.where(inside, placed[dn], edge[...]).astype(bf16)
        copies.append(
            pltpu.make_async_copy(
                out.at[dn],
                nfoot.at[8 * dn : 8 * dn + 16, LOW * dn : LOW * dn + BAND],
                sem.at[2 + dn],
            )
        )
        copies[-1].start()
    for copy in copies:
        copy.wait()


SMEM = pl.BlockSpec(memory_space=pltpu.SMEM)
VMEM = pl.BlockSpec(memory_space=pltpu.VMEM)
LIMIT = 24 * 1024 * 1024


def shape(*dims, dtype=bf16):
    return jax.ShapeDtypeStruct(dims, dtype)


PACKETS = (shape(16, XW), shape(16, XW), shape(16, CW), shape(16, CW))
HBM = pl.BlockSpec(memory_space=pltpu.HBM)


def call(kernel, outs, ins, out_specs, scratch, flops, aliases={}):
    return pl.pallas_call(
        kernel,
        out_shape=outs,
        in_specs=ins,
        out_specs=out_specs,
        scratch_shapes=scratch,
        input_output_aliases=aliases,
        compiler_params=pltpu.CompilerParams(vmem_limit_bytes=LIMIT),
        cost_estimate=pl.CostEstimate(flops=flops, bytes_accessed=1 << 20, transcendentals=0),
    )


def swap(value, axis, parity):
    count = lax.axis_size(axis)
    pairs = []
    for i in range(parity, count - 1, 2):
        pairs += [(i, i + 1), (i + 1, i)]
    return lax.ppermute(value, axis, pairs)


def exchange(xa, xb, va, vb):
    rxb = swap(xb, "px", 1)
    rxa = swap(xa, "px", 0)
    yb = jnp.concatenate([vb, rxa[:, CW : 2 * CW], rxb[:, CW : 2 * CW]], axis=1)
    ya = jnp.concatenate([va, rxa[:, 0:CW], rxb[:, 0:CW]], axis=1)
    ryb = swap(yb, "py", 1)
    rya = swap(ya, "py", 0)
    return rxa, rxb, rya, ryb


def body(
    residual, footprints, traces, merge_pairs, pair_counts, comp_counts, row_inter, col_inter
):
    res = residual[0, 0]
    foot = footprints[0, 0]
    tr = traces[0, 0]
    table = merge_pairs[0, 0]
    wide = jnp.tile(table.T, (1, CH // MP))
    rows, cols = lax.axis_size("py"), lax.axis_size("px")
    res, foot, tr, row_far, col_far = (
        pltpu.with_memory_space_constraint(v, pltpu.HBM)
        for v in (res, foot, tr, row_inter, col_inter)
    )
    dma = pltpu.SemaphoreType.DMA
    i32 = jnp.int32
    geo_scratch = [pltpu.SMEM((1, CH), i32), dma((1,))]

    packets = call(
        pack_kernel,
        PACKETS,
        [HBM] * 2,
        (VMEM,) * 4,
        [pltpu.VMEM((32, NPIX), bf16), pltpu.VMEM((32, F), bf16), dma((2,))],
        1 << 24,
    )(foot, tr)
    rxa, rxb, rya, ryb = exchange(*packets)

    def own(*refs):
        own_kernel(rows, cols, *refs)

    half = (shape(HALF, F), shape(F, HALF), shape(MP, HALF, dtype=f32))
    *prepared, slots, across, geo = call(
        own,
        half
        + (
            shape(MP, F, dtype=f32),
            shape(MP, CH, dtype=i32),
            shape(8, CH, dtype=i32),
            shape(1, CH, dtype=i32),
        ),
        [SMEM] + [HBM] * 4 + [VMEM] * 2,
        (VMEM,) * 7,
        [
            pltpu.VMEM((K, F), bf16),
            pltpu.SMEM((rows - 1,), i32),
            pltpu.SMEM((cols - 1,), i32),
            dma((3,)),
            dma((4,)),
        ],
        1 << 24,
    )(pair_counts, row_far, col_far, res, tr, table, wide)

    placed = call(
        side_kernel,
        half
        + (shape(MP, NPIX, dtype=f32), shape(MP, NPIX, dtype=f32), shape(MP, F, dtype=f32)),
        [HBM] * 2 + [VMEM] * 5,
        (VMEM,) * 6,
        [pltpu.VMEM((K, NPIX), bf16), pltpu.SMEM((1, CH), i32), dma((2,)), dma((4,))],
        1 << 24,
    )(res, foot, geo, prepared[-1], slots, rxa, rxb)

    xa, xb, va, vb, merged, mtrace = call(
        refit_kernel,
        PACKETS + (shape(MP, NPIX), shape(MP, F)),
        [VMEM] * 15,
        (VMEM,) * 6,
        [pltpu.VMEM((MP, NPIX), f32), pltpu.VMEM((6, MP, PBW), bf16)] + geo_scratch,
        1 << 28,
    )(geo, *prepared, slots, across, *placed, rya, ryb)
    oxa, oxb, oya, oyb = exchange(xa, xb, va, vb)

    *partial, corr = call(
        before_kernel,
        (
            shape(K, NPIX),
            shape(K, F, dtype=f32),
            shape(16, BAND, dtype=f32),
            shape(16, BAND, dtype=f32),
            shape(BORDER, K, dtype=f32),
        ),
        [SMEM] + [HBM] * 2 + [VMEM] * 10,
        (VMEM,) * 5,
        [
            pltpu.VMEM((K, NPIX), bf16),
            pltpu.VMEM((K, F), bf16),
            pltpu.SMEM((1, CH), i32),
            dma((3,)),
        ],
        1 << 24,
    )(comp_counts, foot, tr, geo, across, merged, mtrace, rxa, rxb, rya, ryb, oxa, oxb)

    nfoot, ntrace = call(
        final_kernel,
        (shape(K, NPIX), shape(K, F)),
        [VMEM, HBM] + [VMEM] * 5,
        (HBM, HBM),
        [
            pltpu.VMEM((2, 16, BAND), f32),
            pltpu.VMEM((2, 16, 2 * CH), f32),
            pltpu.VMEM((6, 16, PBW), bf16),
            pltpu.VMEM((2, 16, BAND), bf16),
            pltpu.VMEM((K, F), bf16),
            pltpu.SMEM((1, CH), i32),
            dma((4,)),
        ],
        1 << 26,
        {1: 0},
    )(geo, *partial, oya, oyb)
    return nfoot[None, None], ntrace[None, None], corr.T[None, None]


def solution(mesh):
    in_specs = (
        P("py", "px", None, None),
        P("py", "px", None, None),
        P("py", "px", None, None),
        P("py", "px", None, None),
        P("py", "px"),
        P("py", "px"),
        P(),
        P(),
    )
    out_specs = (P("py", "px", None, None), P("py", "px", None, None), P("py", "px", None, None))
    return jax.shard_map(body, mesh=mesh, in_specs=in_specs, out_specs=out_specs, check_vma=False)
```

```python
import jax
import jax.numpy as jnp
from jax import lax
from jax.experimental import pallas as pl
from jax.experimental.pallas import tpu as pltpu
from jax.sharding import PartitionSpec as P


PH = 64
PW = 64
NPIX = PH * PW
K = 40
NBR = 3
BORDER = 24
MP = 16
F = 128
ITERS = 4
OV_HI = 24
epsilon = 1e-05

BAND = OV_HI * PW
LOW = NPIX - BAND
CW = BAND // 4
EW = 896
XW = 2 * CW + EW
CH = 128
PAD = 9
PBW = (PAD + 12 + PAD) * CH

f32 = jnp.float32
bf16 = jnp.bfloat16


def iota(shape, dim):
    return lax.broadcasted_iota(jnp.int32, shape, dim)


def sides():
    row = lax.axis_index("py")
    col = lax.axis_index("px")
    sy = 1 - 2 * lax.rem(row, 2)
    sx = 1 - 2 * lax.rem(col, 2)
    return row, col, (sy, -sy), (sx, -sx)


def direction(dy, dx):
    flat = (dy + 1) * 3 + dx + 1
    return flat - (flat > 4).astype(jnp.int32) if not isinstance(flat, int) else flat - (flat > 4)


def hot(mask):
    return jnp.where(mask, 1.0, 0.0).astype(bf16)


def dot(a, b):
    return jnp.dot(a, b, preferred_element_type=f32)


def band_start(dy):
    return jnp.where(dy > 0, LOW, 0)


def pack_rows(pick, pieces, tail):
    return dot(pick, jnp.concatenate(pieces + [tail], axis=0)).astype(bf16)


def pixel_shift(dy, dx, geo):
    ri = jnp.where(dy > 0, geo[0, 1], geo[0, 0])
    ci = jnp.where(dx > 0, geo[0, 3], geo[0, 2])
    return dy * (OV_HI - ri), dx * (PW - ci)


def column_matrix(ox):
    i = iota((CH, CH), 0)
    o = iota((CH, CH), 1)
    x = (o & (PW - 1)) - ox
    return hot((i == o - ox) & (x >= 0) & (x < PW))


def band_matrix(odd, ox):
    i = iota((2 * CH, CH), 0)
    o = iota((2 * CH, CH), 1)
    x = (o & (PW - 1)) - ox
    return hot((i == o + CH - PW * odd - ox) & (x >= 0) & (x < PW))


def place_whole(whole, ox):
    stack = jnp.concatenate(
        [whole[:, CH * m : CH * (m + 1)] for m in range(32)], axis=0
    ).astype(bf16)
    return dot(stack, column_matrix(ox))


def receive_sides(select, n, xs, sx, geo, ready):
    tail = jnp.zeros((n, 2 * CH), f32)
    whole = None
    taken = [dot(select(direction(0, sx[t])), xs[t][:, 2 * CW : XW]) for t in range(2)]
    ready()
    for t, picked in enumerate(taken):
        full = jnp.concatenate(
            [picked[n * g : n * (g + 1)] for g in range(4)] + [picked[4 * n :, 0:512]], axis=1
        )
        tail = tail + picked[4 * n :, 512 : 512 + 2 * CH]
        _, ox = pixel_shift(0, sx[t], geo)
        moved = place_whole(full, ox)
        whole = moved if whole is None else whole + moved
    return whole, tail


def clear_pads(pbuf):
    pbuf[:, :, 0 : PAD * CH] = jnp.zeros(pbuf.shape[:2] + (PAD * CH,), bf16)
    pbuf[:, :, PAD * CH + BAND :] = jnp.zeros(pbuf.shape[:2] + (PBW - PAD * CH - BAND,), bf16)


def receive_bands(selects, n, ys, pbuf, sy, sx, geo, ready):
    steps = (0, sx[0], sx[1])
    picked = [
        [
            dot(selects[u](direction(sy[u], dx)), ys[u][:, CW * j : CW * (j + 1)])
            for j, dx in enumerate(steps)
        ]
        for u in range(2)
    ]
    clear_pads(pbuf)
    ready()
    for u in range(2):
        for j in range(3):
            for g in range(4):
                at = PAD * CH + CW * g
                pbuf[3 * u + j, :, at : at + CW] = picked[u][j][n * g : n * (g + 1)].astype(bf16)
    out = []
    for u in range(2):
        moved = None
        tail = jnp.zeros((n, 2 * CH), f32)
        for j, dx in enumerate(steps):
            shift, ox = pixel_shift(sy[u], dx, geo)
            first = (PAD - 1 - (shift >> 1)) * CH
            stack = jnp.concatenate(
                [
                    pbuf[3 * u + j, :, pl.ds(pl.multiple_of(first + CH * m, CH), 2 * CH)]
                    for m in range(12)
                ],
                axis=0,
            )
            one = dot(stack, band_matrix(shift & 1, ox))
            moved = one if moved is None else moved + one
            tail = tail + picked[u][j][4 * n :, 0 : 2 * CH]
        out.append((moved, tail))
    return out


def begin(*copies):
    loads = [pltpu.make_async_copy(*copy) for copy in copies]
    for load in loads:
        load.start()

    def ready():
        for load in loads:
            load.wait()

    return ready


def send_all(pick, src, tail_narrow, tail_wide, outs, sy, sx):
    xa, xb, va, vb = outs

    def band_seg(dy, dx):
        start = band_start(dy)
        pieces = [
            src[:, pl.ds(pl.multiple_of(start + CW * g, CH), CW)] for g in range(4)
        ]
        return pack_rows(pick(direction(dy, dx)), pieces, tail_narrow)

    def whole_seg(dx):
        pieces = [src[:, EW * g : EW * (g + 1)] for g in range(4)]
        last = jnp.concatenate([src[:, 4 * EW : NPIX], tail_wide], axis=1)
        return pack_rows(pick(direction(0, dx)), pieces, last)

    for t, out in enumerate((xa, xb)):
        out[:, 0:CW] = band_seg(sy[0], sx[t])
        out[:, CW : 2 * CW] = band_seg(sy[1], sx[t])
        out[:, 2 * CW : XW] = whole_seg(sx[t])
    va[...] = band_seg(sy[0], 0)
    vb[...] = band_seg(sy[1], 0)


def group_of(j):
    g = (j >= 3).astype(jnp.int32) + (j >= 6) + (j >= 9) + (j >= 12)
    return g, j - 3 * g


def pack_kernel(foot, tr, xa, xb, va, vb, src, trs, sem):
    ready = begin(
        (foot.at[0:32, :], src, sem.at[0]), (tr.at[0:32, :], trs, sem.at[1])
    )
    _, _, sy, sx = sides()
    j = iota((16, 160), 0)
    kk = iota((16, 160), 1)
    g, s = group_of(j)
    same = ((kk >> 5) == g) & (j < 15)
    comp = (kk & 31) - s

    def pick(d):
        return hot(same & (comp == 3 * d))

    ready()
    tail = jnp.concatenate([trs[...], jnp.zeros((32, 2 * CH), bf16)], axis=1)
    send_all(pick, src, tail, tail, (xa, xb, va, vb), sy, sx)


def slot_select(table):
    j5 = iota((5 * MP, 16), 1)
    g5 = iota((5 * MP, 16), 0) >> 4
    s5 = j5 - 3 * g5
    idx5 = jnp.concatenate([table[:, 1:2]] * 5, axis=0)
    fits = (s5 >= 0) & (s5 < 3)

    def select(d):
        return hot(fits & (idx5 == 3 * d + s5))

    return select


NT = (((1,), (1,)), ((), ()))


HEAD = 512


def load_part(res_in, start, res, sem):
    width = 512
    return [
        begin(
            (
                res_in.at[start + width * n : start + width * (n + 1), :],
                res.at[width * n : width * (n + 1), :],
                sem.at[n],
            )
        )
        for n in range(res.shape[0] // width)
    ]


def turn_part(loads, c_own, res, rest, first):
    width = 512
    eye = hot(iota((CH, CH), 0) == iota((CH, CH), 1))
    both = jnp.concatenate([c_own.astype(bf16), eye], axis=0)
    for n, load in enumerate(loads):
        lanes = slice(width * n, width * (n + 1))
        load()
        turned = lax.dot_general(both, res[lanes, :], NT, preferred_element_type=f32)
        first[:, lanes] = turned[0:MP]
        rest[:, lanes] = turned[MP:].astype(bf16)


def own_kernel(
    rows, cols, count, row_in, col_in, res_in, tr_in, table, wide,
    res, rest, first, ctr, slots, across, geo, tr, row_ref, col_ref, sem, rsem,
):
    small = begin((tr_in, tr, sem.at[0]))
    loads = load_part(res_in, 0, res, rsem)
    scalars = begin((row_in, row_ref, sem.at[1]), (col_in, col_ref, sem.at[2]))
    row, col, _, _ = sides()
    total = count[0, 0]
    ids = table[:, 0:1]
    live = iota((MP, CH), 0) < total
    idx = NBR * table[:, 1:2] + table[:, 2:3]
    place = iota((MP, CH), 1)
    dead = jnp.where(live, jnp.where(place == 0, ids, idx), -100)
    slots[...] = jnp.where(place == 2, ids, dead)
    line = iota((8, CH), 0)
    alive = (iota((8, CH), 1) & 15) < total
    pair = NBR * wide[1:2, :] + wide[2:3, :]
    across[...] = jnp.where(alive, jnp.where(line == 0, wide[0:1, :], pair), -100)
    own_hot = hot(ids == iota((MP, K), 1))
    small()
    c_own = dot(own_hot, tr[...])
    ctr[...] = c_own
    turn_part(loads, c_own, res, rest, first)
    scalars()
    up = row_ref[jnp.clip(row - 1, 0, rows - 2)]
    down = row_ref[jnp.clip(row, 0, rows - 2)]
    left = col_ref[jnp.clip(col - 1, 0, cols - 2)]
    right = col_ref[jnp.clip(col, 0, cols - 2)]
    lane = iota((1, CH), 1)
    geo[...] = jnp.where(
        lane == 0, up, jnp.where(lane == 1, down, jnp.where(lane == 2, left, right))
    )


def side_kernel(
    res_in, foot_in, geo_in, ctr, slots, rxa, rxb, res, rest, first, own, side, crem, foot, geo, sem, rsem
):
    loads = load_part(res_in, HEAD, res, rsem)
    load = begin((foot_in, foot, sem.at[1]))
    ready = begin((geo_in, geo, sem.at[0]))
    _, _, _, sx = sides()
    own_hot = hot(slots[:, 2:3] == iota((MP, K), 1))
    whole, tail = receive_sides(slot_select(slots), MP, (rxa, rxb), sx, geo, ready)
    crem[...] = tail[:, 0:F]
    for m in range(32):
        side[:, CH * m : CH * (m + 1)] = whole[MP * m : MP * (m + 1)]
    turn_part(loads, ctr[...], res, rest, first)
    load()
    own[...] = dot(own_hot, foot[...])


def refit_kernel(
    geo_in, res_l, rest_l, first_l, ctr, slots, wide, res_h, rest_h, first_h, own, side, crem, rya, ryb,
    xa, xb, va, vb, merged, mtrace, acc, pbuf, geo, sem,
):
    ready = begin((geo_in, geo, sem.at[0]))
    _, _, sy, sx = sides()
    live = slots[:, 1:2] >= 0
    select = slot_select(slots)
    acc[...] = side[...]
    c_own = ctr[...]
    c_rem = crem[...]
    bands = receive_bands((select, select), MP, (rya, ryb), pbuf, sy, sx, geo, ready)
    for u, (moved, tail) in enumerate(bands):
        c_rem = c_rem + tail[:, 0:F]
        start = band_start(sy[u])
        for m in range(12):
            lanes = pl.ds(pl.multiple_of(start + CH * m, CH), CH)
            acc[:, lanes] += moved[MP * m : MP * (m + 1)]
    trace = c_own
    step = 512
    for it in range(ITERS):
        tb = trace.astype(bf16)
        co = jnp.sum(c_own * trace, axis=1, keepdims=True)
        cr = jnp.sum(c_rem * trace, axis=1, keepdims=True)
        scale = 1.0 / (jnp.sum(trace * trace, axis=1, keepdims=True) + epsilon * F)
        lanes = [slice(step * n, step * (n + 1)) for n in range(NPIX // step)]
        cuts = [
            [slice(step * n, step * (n + 1)) for n in range(size // step)] for size in (HEAD, NPIX - HEAD)
        ]
        if it == 0:
            across = [f[:, cut] for f, some in zip((first_l, first_h), cuts) for cut in some]
        else:
            across = [dot(tb, r[:, cut]) for r, some in zip((rest_l, rest_h), cuts) for cut in some]
        sa = jnp.zeros((MP, CH), f32)
        sr = jnp.zeros((MP, CH), f32)
        ss = jnp.zeros((MP, CH), f32)
        shapes = []
        for n, cut in enumerate(lanes):
            ao = own[:, cut]
            ar = acc[:, cut]
            now = jnp.maximum(across[n] + ao * co + ar * cr, 0.0) * scale
            shapes.append(now.astype(bf16))
            if it == ITERS - 1:
                merged[:, cut] = jnp.where(live, now, 0.0).astype(bf16)
            pa = ao * now
            pr = ar * now
            ps = now * now
            for q in range(step // CH):
                part = slice(CH * q, CH * (q + 1))
                sa = sa + pa[:, part]
                sr = sr + pr[:, part]
                ss = ss + ps[:, part]
        parts = [r[cut, :] for r, some in zip((res_l, res_h), cuts) for cut in some]
        down = sum(dot(now, part) for now, part in zip(shapes, parts))
        down = (
            down
            + c_own * jnp.sum(sa, axis=1, keepdims=True)
            + c_rem * jnp.sum(sr, axis=1, keepdims=True)
        )
        trace = jnp.maximum(down, 0.0) / (jnp.sum(ss, axis=1, keepdims=True) + epsilon * NPIX)
    tout = jnp.where(live, trace, 0.0).astype(bf16)
    mtrace[...] = tout
    j = iota((16, 5 * MP), 0)
    kk = iota((16, 5 * MP), 1)
    g, s = group_of(j)
    same = ((kk >> 4) == g) & (j < 15)
    comp = wide[1:2, 0 : 5 * MP] - s

    def pick(d):
        return hot(same & (comp == 3 * d))

    ones = jnp.ones((MP, CH), bf16)
    blank = jnp.zeros((MP, CH), bf16)
    tail = jnp.concatenate([tout, ones, blank], axis=1)
    send_all(pick, merged, tail, tail, (xa, xb, va, vb), sy, sx)


def correlate(alive, tr, rxa, rxb, rya, ryb, out, sy, sx):
    k = iota((BORDER, 16), 0)
    j = iota((BORDER, 16), 1)
    s = j - 12
    fits = (s >= 0) & (s < 3)
    z = jnp.zeros((BORDER, F), f32)
    for t, ref in enumerate((rxa, rxb)):
        at = 2 * CW + 512
        z = z + dot(hot(fits & (k == 3 * direction(0, sx[t]) + s)), ref[:, at : at + F])
    for u, ref in enumerate((rya, ryb)):
        for q, dx in enumerate((0, sx[0], sx[1])):
            z = z + dot(hot(fits & (k == 3 * direction(sy[u], dx) + s)), ref[:, CW * q : CW * q + F])
    x = tr.astype(f32)
    x = x - jnp.mean(x, axis=1, keepdims=True)
    z = z - jnp.mean(z, axis=1, keepdims=True)
    high = lax.Precision.HIGHEST
    cov = lax.dot_general(z, x, NT, precision=high, preferred_element_type=f32) / F
    vz = jnp.mean(z * z, axis=1, keepdims=True)
    ones = jnp.ones((8, F), f32)
    vx = lax.dot_general(ones, x * x, NT, precision=high, preferred_element_type=f32)[0:1] / F
    out[...] = jnp.where(alive, cov / jnp.sqrt((vx + epsilon) * (vz + epsilon)), 0.0)


def row_select(n, first):
    j5 = iota((5 * n, 16), 1)
    r5 = iota((5 * n, 16), 0)
    s5 = j5 - 3 * (r5 >> 4)
    k5 = (r5 & 15) + first
    fits = (s5 >= 0) & (s5 < 3)

    def select(d):
        return hot(fits & (k5 == 3 * d + s5))

    return select


def before_kernel(
    comp, foot_in, tr_in, geo_in, wide, merged, mtrace, oxa, oxb, oya, oyb, rxa, rxb,
    base, tbase, upper, lower, corr, foot, tr, geo, sem,
):
    quick = begin((geo_in, geo, sem.at[0]))
    ready = begin((tr_in, tr, sem.at[1]), (foot_in, foot, sem.at[2]))
    _, _, sy, sx = sides()
    n = 16
    whole, tail = receive_sides(row_select(n, 8), n, (rxa, rxb), sx, geo, quick)
    flag = tail[:, CH : CH + 1] > 0.5
    k = iota((n, 1), 0) + 8
    x_lo = jnp.where(k >= 12, PW - geo[0, 3], 0)
    x_hi = jnp.where(flag, jnp.where(k < 12, geo[0, 2], PW), 0)
    x = iota((1, CH), 1) & (PW - 1)
    inside = (x >= x_lo) & (x < x_hi)
    own_hot = hot(iota((K - BORDER, MP), 0) + BORDER == wide[0:1, 0:MP])
    hit = jnp.sum(own_hot.astype(f32), axis=1, keepdims=True) > 0.5
    ready()
    correlate(iota((1, K), 1) < comp[0, 0], tr[...], oxa, oxb, oya, oyb, corr, sy, sx)
    alive = iota((K - BORDER, 1), 0) + BORDER < comp[0, 0]
    step = 512
    for b in range(NPIX // step):
        lanes = slice(step * b, step * (b + 1))
        mine = foot[:, lanes].astype(f32)
        got = dot(own_hot, merged[:, lanes])
        low = jnp.where(alive, jnp.where(hit, got, mine[BORDER:]), 0.0)
        mid = []
        for q in range(step // CH):
            m = b * (step // CH) + q
            mid.append(
                jnp.where(
                    inside, whole[n * m : n * (m + 1)], mine[8:BORDER, CH * q : CH * (q + 1)]
                )
            )
        mid = jnp.concatenate(mid, axis=1)
        base[:, lanes] = jnp.concatenate([mine[0:8], mid, low], axis=0).astype(bf16)
        if step * b < BAND:
            upper[:, lanes] = jnp.concatenate([mine[0:8], mid[0:8]], axis=0)
        if step * b >= LOW:
            lower[:, step * b - LOW : step * (b + 1) - LOW] = mid
    mine = tr[...].astype(f32)
    mid = jnp.where(flag, tail[:, 0:F], mine[8:BORDER])
    low = jnp.where(alive, jnp.where(hit, dot(own_hot, mtrace[...]), mine[BORDER:]), 0.0)
    tbase[...] = jnp.concatenate([mine[0:8], mid, low], axis=0)


def final_kernel(
    geo_in, base, tbase, upper, lower, rya, ryb,
    nfoot, ntrace, placed, tails, pbuf, out, tout, geo, sem,
):
    ready = begin((geo_in, geo, sem.at[0]))
    _, _, sy, sx = sides()
    n = 16
    downs = [jnp.where(sy[u] > 0, 1, 0) for u in range(2)]
    bands = receive_bands(
        [row_select(n, 8 * dn) for dn in downs], n, (rya, ryb), pbuf, sy, sx, geo, ready
    )
    for dn, (moved, tail) in zip(downs, bands):
        for m in range(12):
            placed[dn, :, CH * m : CH * (m + 1)] = moved[n * m : n * (m + 1)]
        tails[dn] = tail
    mine = tbase[0:BORDER]
    gap = jnp.zeros((8, 2 * CH), f32)
    both = jnp.concatenate([tails[0], gap], axis=0) + jnp.concatenate([gap, tails[1]], axis=0)
    top = jnp.where(both[:, CH : CH + 1] > 0.5, both[:, 0:F], mine)
    tout[...] = jnp.concatenate([top, tbase[BORDER:]], axis=0).astype(bf16)
    copies = [pltpu.make_async_copy(tout, ntrace, sem.at[1])]
    copies[0].start()
    r_up, r_dn, c_lf, c_rt = (geo[0, i] for i in range(4))
    k = iota((n, 1), 0)
    pix = iota((1, BAND), 1)
    y = pix >> 6
    x = pix & (PW - 1)
    for dn, edge in enumerate((upper, lower)):
        j = k - 7 * dn
        flag = tails[dn, :, CH : CH + 1] > 0.5
        x_lo = jnp.where(j >= 6, PW - c_rt, 0)
        x_hi = jnp.where(flag, jnp.where(j < 3, c_lf, PW), 0)
        y_ok = (y < r_up) if dn == 0 else (y >= OV_HI - r_dn)
        inside = y_ok & (x >= x_lo) & (x < x_hi)
        out[dn] = jnp.where(inside, placed[dn], edge[...]).astype(bf16)
        copies.append(
            pltpu.make_async_copy(
                out.at[dn],
                nfoot.at[8 * dn : 8 * dn + 16, LOW * dn : LOW * dn + BAND],
                sem.at[2 + dn],
            )
        )
        copies[-1].start()
    for copy in copies:
        copy.wait()


SMEM = pl.BlockSpec(memory_space=pltpu.SMEM)
VMEM = pl.BlockSpec(memory_space=pltpu.VMEM)
LIMIT = 24 * 1024 * 1024


def shape(*dims, dtype=bf16):
    return jax.ShapeDtypeStruct(dims, dtype)


PACKETS = (shape(16, XW), shape(16, XW), shape(16, CW), shape(16, CW))
HBM = pl.BlockSpec(memory_space=pltpu.HBM)


def call(kernel, outs, ins, out_specs, scratch, flops, aliases={}):
    return pl.pallas_call(
        kernel,
        out_shape=outs,
        in_specs=ins,
        out_specs=out_specs,
        scratch_shapes=scratch,
        input_output_aliases=aliases,
        compiler_params=pltpu.CompilerParams(vmem_limit_bytes=LIMIT),
        cost_estimate=pl.CostEstimate(flops=flops, bytes_accessed=1 << 20, transcendentals=0),
    )


def swap(value, axis, parity):
    count = lax.axis_size(axis)
    pairs = []
    for i in range(parity, count - 1, 2):
        pairs += [(i, i + 1), (i + 1, i)]
    return lax.ppermute(value, axis, pairs)


def exchange(xa, xb, va, vb):
    rxb = swap(xb, "px", 1)
    rxa = swap(xa, "px", 0)
    yb = jnp.concatenate([vb, rxa[:, CW : 2 * CW], rxb[:, CW : 2 * CW]], axis=1)
    ya = jnp.concatenate([va, rxa[:, 0:CW], rxb[:, 0:CW]], axis=1)
    ryb = swap(yb, "py", 1)
    rya = swap(ya, "py", 0)
    return rxa, rxb, rya, ryb


def body(
    residual, footprints, traces, merge_pairs, pair_counts, comp_counts, row_inter, col_inter
):
    res = residual[0, 0]
    foot = footprints[0, 0]
    tr = traces[0, 0]
    table = merge_pairs[0, 0]
    wide = jnp.tile(table.T, (1, CH // MP))
    rows, cols = lax.axis_size("py"), lax.axis_size("px")
    res, foot, tr, row_far, col_far = (
        pltpu.with_memory_space_constraint(v, pltpu.HBM)
        for v in (res, foot, tr, row_inter, col_inter)
    )
    dma = pltpu.SemaphoreType.DMA
    i32 = jnp.int32
    geo_scratch = [pltpu.SMEM((1, CH), i32), dma((1,))]

    packets = call(
        pack_kernel,
        PACKETS,
        [HBM] * 2,
        (VMEM,) * 4,
        [pltpu.VMEM((32, NPIX), bf16), pltpu.VMEM((32, F), bf16), dma((2,))],
        1 << 24,
    )(foot, tr)
    rxa, rxb, rya, ryb = exchange(*packets)

    def own(*refs):
        own_kernel(rows, cols, *refs)

    def part(size):
        return (shape(size, F), shape(F, size), shape(MP, size, dtype=f32))

    *prepared, slots, across, geo = call(
        own,
        part(HEAD)
        + (
            shape(MP, F, dtype=f32),
            shape(MP, CH, dtype=i32),
            shape(8, CH, dtype=i32),
            shape(1, CH, dtype=i32),
        ),
        [SMEM] + [HBM] * 4 + [VMEM] * 2,
        (VMEM,) * 7,
        [
            pltpu.VMEM((K, F), bf16),
            pltpu.SMEM((rows - 1,), i32),
            pltpu.SMEM((cols - 1,), i32),
            dma((3,)),
            dma((HEAD // 512,)),
        ],
        1 << 24,
    )(pair_counts, row_far, col_far, res, tr, table, wide)

    placed = call(
        side_kernel,
        part(NPIX - HEAD)
        + (shape(MP, NPIX, dtype=f32), shape(MP, NPIX, dtype=f32), shape(MP, F, dtype=f32)),
        [HBM] * 2 + [VMEM] * 5,
        (VMEM,) * 6,
        [pltpu.VMEM((K, NPIX), bf16), pltpu.SMEM((1, CH), i32), dma((2,)), dma(((NPIX - HEAD) // 512,))],
        1 << 24,
    )(res, foot, geo, prepared[-1], slots, rxa, rxb)

    xa, xb, va, vb, merged, mtrace = call(
        refit_kernel,
        PACKETS + (shape(MP, NPIX), shape(MP, F)),
        [VMEM] * 15,
        (VMEM,) * 6,
        [pltpu.VMEM((MP, NPIX), f32), pltpu.VMEM((6, MP, PBW), bf16)] + geo_scratch,
        1 << 28,
    )(geo, *prepared, slots, across, *placed, rya, ryb)
    oxa, oxb, oya, oyb = exchange(xa, xb, va, vb)

    *partial, corr = call(
        before_kernel,
        (
            shape(K, NPIX),
            shape(K, F, dtype=f32),
            shape(16, BAND, dtype=f32),
            shape(16, BAND, dtype=f32),
            shape(BORDER, K, dtype=f32),
        ),
        [SMEM] + [HBM] * 2 + [VMEM] * 10,
        (VMEM,) * 5,
        [
            pltpu.VMEM((K, NPIX), bf16),
            pltpu.VMEM((K, F), bf16),
            pltpu.SMEM((1, CH), i32),
            dma((3,)),
        ],
        1 << 24,
    )(comp_counts, foot, tr, geo, across, merged, mtrace, rxa, rxb, rya, ryb, oxa, oxb)

    nfoot, ntrace = call(
        final_kernel,
        (shape(K, NPIX), shape(K, F)),
        [VMEM, HBM] + [VMEM] * 5,
        (HBM, HBM),
        [
            pltpu.VMEM((2, 16, BAND), f32),
            pltpu.VMEM((2, 16, 2 * CH), f32),
            pltpu.VMEM((6, 16, PBW), bf16),
            pltpu.VMEM((2, 16, BAND), bf16),
            pltpu.VMEM((K, F), bf16),
            pltpu.SMEM((1, CH), i32),
            dma((4,)),
        ],
        1 << 26,
        {1: 0},
    )(geo, *partial, oya, oyb)
    return nfoot[None, None], ntrace[None, None], corr.T[None, None]


def solution(mesh):
    in_specs = (
        P("py", "px", None, None),
        P("py", "px", None, None),
        P("py", "px", None, None),
        P("py", "px", None, None),
        P("py", "px"),
        P("py", "px"),
        P(),
        P(),
    )
    out_specs = (P("py", "px", None, None), P("py", "px", None, None), P("py", "px", None, None))
    return jax.shard_map(body, mesh=mesh, in_specs=in_specs, out_specs=out_specs, check_vma=False)
```

```python
import jax
import jax.numpy as jnp
from jax import lax
from jax.experimental import pallas as pl
from jax.experimental.pallas import tpu as pltpu
from jax.sharding import PartitionSpec as P


PH = 64
PW = 64
NPIX = PH * PW
K = 40
NBR = 3
BORDER = 24
MP = 16
F = 128
ITERS = 4
OV_HI = 24
epsilon = 1e-05

BAND = OV_HI * PW
LOW = NPIX - BAND
CW = BAND // 4
EW = 896
XW = 2 * CW + EW
CH = 128
PAD = 9
PBW = (PAD + 12 + PAD) * CH

f32 = jnp.float32
bf16 = jnp.bfloat16


def iota(shape, dim):
    return lax.broadcasted_iota(jnp.int32, shape, dim)


def sides():
    row = lax.axis_index("py")
    col = lax.axis_index("px")
    sy = 1 - 2 * lax.rem(row, 2)
    sx = 1 - 2 * lax.rem(col, 2)
    return row, col, (sy, -sy), (sx, -sx)


def direction(dy, dx):
    flat = (dy + 1) * 3 + dx + 1
    return flat - (flat > 4).astype(jnp.int32) if not isinstance(flat, int) else flat - (flat > 4)


def hot(mask):
    return jnp.where(mask, 1.0, 0.0).astype(bf16)


def dot(a, b):
    return jnp.dot(a, b, preferred_element_type=f32)


def band_start(dy):
    return jnp.where(dy > 0, LOW, 0)


def pack_rows(pick, pieces, tail):
    return dot(pick, jnp.concatenate(pieces + [tail], axis=0)).astype(bf16)


def pixel_shift(dy, dx, geo):
    ri = jnp.where(dy > 0, geo[0, 1], geo[0, 0])
    ci = jnp.where(dx > 0, geo[0, 3], geo[0, 2])
    return dy * (OV_HI - ri), dx * (PW - ci)


def column_matrix(ox):
    i = iota((CH, CH), 0)
    o = iota((CH, CH), 1)
    x = (o & (PW - 1)) - ox
    return hot((i == o - ox) & (x >= 0) & (x < PW))


def band_matrix(odd, ox):
    i = iota((2 * CH, CH), 0)
    o = iota((2 * CH, CH), 1)
    x = (o & (PW - 1)) - ox
    return hot((i == o + CH - PW * odd - ox) & (x >= 0) & (x < PW))


def place_whole(whole, ox):
    stack = jnp.concatenate(
        [whole[:, CH * m : CH * (m + 1)] for m in range(32)], axis=0
    ).astype(bf16)
    return dot(stack, column_matrix(ox))


def receive_sides(select, n, xs, sx, geo, ready):
    tail = jnp.zeros((n, 2 * CH), f32)
    whole = None
    taken = [dot(select(direction(0, sx[t])), xs[t][:, 2 * CW : XW]) for t in range(2)]
    ready()
    for t, picked in enumerate(taken):
        full = jnp.concatenate(
            [picked[n * g : n * (g + 1)] for g in range(4)] + [picked[4 * n :, 0:512]], axis=1
        )
        tail = tail + picked[4 * n :, 512 : 512 + 2 * CH]
        _, ox = pixel_shift(0, sx[t], geo)
        moved = place_whole(full, ox)
        whole = moved if whole is None else whole + moved
    return whole, tail


def clear_pads(pbuf):
    pbuf[:, :, 0 : PAD * CH] = jnp.zeros(pbuf.shape[:2] + (PAD * CH,), bf16)
    pbuf[:, :, PAD * CH + BAND :] = jnp.zeros(pbuf.shape[:2] + (PBW - PAD * CH - BAND,), bf16)


def receive_bands(selects, n, ys, pbuf, sy, sx, geo, ready):
    steps = (0, sx[0], sx[1])
    picked = [
        [
            dot(selects[u](direction(sy[u], dx)), ys[u][:, CW * j : CW * (j + 1)])
            for j, dx in enumerate(steps)
        ]
        for u in range(2)
    ]
    clear_pads(pbuf)
    ready()
    for u in range(2):
        for j in range(3):
            for g in range(4):
                at = PAD * CH + CW * g
                pbuf[3 * u + j, :, at : at + CW] = picked[u][j][n * g : n * (g + 1)].astype(bf16)
    out = []
    for u in range(2):
        moved = None
        tail = jnp.zeros((n, 2 * CH), f32)
        for j, dx in enumerate(steps):
            shift, ox = pixel_shift(sy[u], dx, geo)
            first = (PAD - 1 - (shift >> 1)) * CH
            stack = jnp.concatenate(
                [
                    pbuf[3 * u + j, :, pl.ds(pl.multiple_of(first + CH * m, CH), 2 * CH)]
                    for m in range(12)
                ],
                axis=0,
            )
            one = dot(stack, band_matrix(shift & 1, ox))
            moved = one if moved is None else moved + one
            tail = tail + picked[u][j][4 * n :, 0 : 2 * CH]
        out.append((moved, tail))
    return out


def begin(*copies):
    loads = [pltpu.make_async_copy(*copy) for copy in copies]
    for load in loads:
        load.start()

    def ready():
        for load in loads:
            load.wait()

    return ready


def send_all(pick, src, tail_narrow, tail_wide, outs, sy, sx):
    xa, xb, va, vb = outs

    def band_seg(dy, dx):
        start = band_start(dy)
        pieces = [
            src[:, pl.ds(pl.multiple_of(start + CW * g, CH), CW)] for g in range(4)
        ]
        return pack_rows(pick(direction(dy, dx)), pieces, tail_narrow)

    def whole_seg(dx):
        pieces = [src[:, EW * g : EW * (g + 1)] for g in range(4)]
        last = jnp.concatenate([src[:, 4 * EW : NPIX], tail_wide], axis=1)
        return pack_rows(pick(direction(0, dx)), pieces, last)

    for t, out in enumerate((xa, xb)):
        out[:, 0:CW] = band_seg(sy[0], sx[t])
        out[:, CW : 2 * CW] = band_seg(sy[1], sx[t])
        out[:, 2 * CW : XW] = whole_seg(sx[t])
    va[...] = band_seg(sy[0], 0)
    vb[...] = band_seg(sy[1], 0)


def group_of(j):
    g = (j >= 3).astype(jnp.int32) + (j >= 6) + (j >= 9) + (j >= 12)
    return g, j - 3 * g


def pack_kernel(foot, tr, xa, xb, va, vb, src, trs, sem):
    ready = begin(
        (foot.at[0:32, :], src, sem.at[0]), (tr.at[0:32, :], trs, sem.at[1])
    )
    _, _, sy, sx = sides()
    j = iota((16, 160), 0)
    kk = iota((16, 160), 1)
    g, s = group_of(j)
    same = ((kk >> 5) == g) & (j < 15)
    comp = (kk & 31) - s

    def pick(d):
        return hot(same & (comp == 3 * d))

    ready()
    tail = jnp.concatenate([trs[...], jnp.zeros((32, 2 * CH), bf16)], axis=1)
    send_all(pick, src, tail, tail, (xa, xb, va, vb), sy, sx)


def slot_select(table):
    j5 = iota((5 * MP, 16), 1)
    g5 = iota((5 * MP, 16), 0) >> 4
    s5 = j5 - 3 * g5
    idx5 = jnp.concatenate([table[:, 1:2]] * 5, axis=0)
    fits = (s5 >= 0) & (s5 < 3)

    def select(d):
        return hot(fits & (idx5 == 3 * d + s5))

    return select


NT = (((1,), (1,)), ((), ()))


HEAD = 512


def load_part(res_in, start, res, sem):
    width = 512
    return [
        begin(
            (
                res_in.at[start + width * n : start + width * (n + 1), :],
                res.at[width * n : width * (n + 1), :],
                sem.at[n],
            )
        )
        for n in range(res.shape[0] // width)
    ]


def turn_part(loads, c_own, res, rest, first):
    width = 512
    eye = hot(iota((CH, CH), 0) == iota((CH, CH), 1))
    both = jnp.concatenate([c_own.astype(bf16), eye], axis=0)
    for n, load in enumerate(loads):
        lanes = slice(width * n, width * (n + 1))
        load()
        turned = lax.dot_general(both, res[lanes, :], NT, preferred_element_type=f32)
        first[:, lanes] = turned[0:MP]
        rest[:, lanes] = turned[MP:].astype(bf16)


def own_kernel(
    rows, cols, row_in, col_in, res_in, tr_in, table,
    res, rest, first, ctr, geo, tr, row_ref, col_ref, sem, rsem,
):
    small = begin((tr_in, tr, sem.at[0]))
    loads = load_part(res_in, 0, res, rsem)
    scalars = begin((row_in, row_ref, sem.at[1]), (col_in, col_ref, sem.at[2]))
    row, col, _, _ = sides()
    own_hot = hot(table[:, 0:1] == iota((MP, K), 1))
    small()
    c_own = dot(own_hot, tr[...])
    ctr[...] = c_own
    turn_part(loads, c_own, res, rest, first)
    scalars()
    up = row_ref[jnp.clip(row - 1, 0, rows - 2)]
    down = row_ref[jnp.clip(row, 0, rows - 2)]
    left = col_ref[jnp.clip(col - 1, 0, cols - 2)]
    right = col_ref[jnp.clip(col, 0, cols - 2)]
    lane = iota((1, CH), 1)
    geo[...] = jnp.where(
        lane == 0, up, jnp.where(lane == 1, down, jnp.where(lane == 2, left, right))
    )


def side_kernel(
    count, res_in, foot_in, geo_in, ctr, table, wide, rxa, rxb,
    res, rest, first, own, side, crem, slots, across, foot, geo, sem, rsem,
):
    loads = load_part(res_in, HEAD, res, rsem)
    load = begin((foot_in, foot, sem.at[1]))
    ready = begin((geo_in, geo, sem.at[0]))
    _, _, _, sx = sides()
    total = count[0, 0]
    ids = table[:, 0:1]
    live = iota((MP, CH), 0) < total
    idx = NBR * table[:, 1:2] + table[:, 2:3]
    slots[...] = jnp.where(live, jnp.where(iota((MP, CH), 1) == 0, ids, idx), -100)
    line = iota((8, CH), 0)
    alive = (iota((8, CH), 1) & 15) < total
    pair = NBR * wide[1:2, :] + wide[2:3, :]
    across[...] = jnp.where(alive, jnp.where(line == 0, wide[0:1, :], pair), -100)
    own_hot = hot(ids == iota((MP, K), 1))
    whole, tail = receive_sides(slot_select(slots), MP, (rxa, rxb), sx, geo, ready)
    crem[...] = tail[:, 0:F]
    for m in range(32):
        side[:, CH * m : CH * (m + 1)] = whole[MP * m : MP * (m + 1)]
    turn_part(loads, ctr[...], res, rest, first)
    load()
    own[...] = dot(own_hot, foot[...])


def refit_kernel(
    geo_in, res_l, rest_l, first_l, ctr, slots, wide, res_h, rest_h, first_h, own, side, crem, rya, ryb,
    xa, xb, va, vb, merged, mtrace, acc, pbuf, geo, sem,
):
    ready = begin((geo_in, geo, sem.at[0]))
    _, _, sy, sx = sides()
    live = slots[:, 1:2] >= 0
    select = slot_select(slots)
    acc[...] = side[...]
    c_own = ctr[...]
    c_rem = crem[...]
    bands = receive_bands((select, select), MP, (rya, ryb), pbuf, sy, sx, geo, ready)
    for u, (moved, tail) in enumerate(bands):
        c_rem = c_rem + tail[:, 0:F]
        start = band_start(sy[u])
        for m in range(12):
            lanes = pl.ds(pl.multiple_of(start + CH * m, CH), CH)
            acc[:, lanes] += moved[MP * m : MP * (m + 1)]
    trace = c_own
    step = 512
    for it in range(ITERS):
        tb = trace.astype(bf16)
        co = jnp.sum(c_own * trace, axis=1, keepdims=True)
        cr = jnp.sum(c_rem * trace, axis=1, keepdims=True)
        scale = 1.0 / (jnp.sum(trace * trace, axis=1, keepdims=True) + epsilon * F)
        lanes = [slice(step * n, step * (n + 1)) for n in range(NPIX // step)]
        cuts = [
            [slice(step * n, step * (n + 1)) for n in range(size // step)] for size in (HEAD, NPIX - HEAD)
        ]
        if it == 0:
            across = [f[:, cut] for f, some in zip((first_l, first_h), cuts) for cut in some]
        else:
            across = [dot(tb, r[:, cut]) for r, some in zip((rest_l, rest_h), cuts) for cut in some]
        sa = jnp.zeros((MP, CH), f32)
        sr = jnp.zeros((MP, CH), f32)
        ss = jnp.zeros((MP, CH), f32)
        shapes = []
        for n, cut in enumerate(lanes):
            ao = own[:, cut]
            ar = acc[:, cut]
            now = jnp.maximum(across[n] + ao * co + ar * cr, 0.0) * scale
            shapes.append(now.astype(bf16))
            if it == ITERS - 1:
                merged[:, cut] = jnp.where(live, now, 0.0).astype(bf16)
            pa = ao * now
            pr = ar * now
            ps = now * now
            for q in range(step // CH):
                part = slice(CH * q, CH * (q + 1))
                sa = sa + pa[:, part]
                sr = sr + pr[:, part]
                ss = ss + ps[:, part]
        parts = [r[cut, :] for r, some in zip((res_l, res_h), cuts) for cut in some]
        down = sum(dot(now, part) for now, part in zip(shapes, parts))
        down = (
            down
            + c_own * jnp.sum(sa, axis=1, keepdims=True)
            + c_rem * jnp.sum(sr, axis=1, keepdims=True)
        )
        trace = jnp.maximum(down, 0.0) / (jnp.sum(ss, axis=1, keepdims=True) + epsilon * NPIX)
    tout = jnp.where(live, trace, 0.0).astype(bf16)
    mtrace[...] = tout
    j = iota((16, 5 * MP), 0)
    kk = iota((16, 5 * MP), 1)
    g, s = group_of(j)
    same = ((kk >> 4) == g) & (j < 15)
    comp = wide[1:2, 0 : 5 * MP] - s

    def pick(d):
        return hot(same & (comp == 3 * d))

    ones = jnp.ones((MP, CH), bf16)
    blank = jnp.zeros((MP, CH), bf16)
    tail = jnp.concatenate([tout, ones, blank], axis=1)
    send_all(pick, merged, tail, tail, (xa, xb, va, vb), sy, sx)


def correlate(alive, tr, rxa, rxb, rya, ryb, out, sy, sx):
    k = iota((BORDER, 16), 0)
    j = iota((BORDER, 16), 1)
    s = j - 12
    fits = (s >= 0) & (s < 3)
    z = jnp.zeros((BORDER, F), f32)
    for t, ref in enumerate((rxa, rxb)):
        at = 2 * CW + 512
        z = z + dot(hot(fits & (k == 3 * direction(0, sx[t]) + s)), ref[:, at : at + F])
    for u, ref in enumerate((rya, ryb)):
        for q, dx in enumerate((0, sx[0], sx[1])):
            z = z + dot(hot(fits & (k == 3 * direction(sy[u], dx) + s)), ref[:, CW * q : CW * q + F])
    x = tr.astype(f32)
    x = x - jnp.mean(x, axis=1, keepdims=True)
    z = z - jnp.mean(z, axis=1, keepdims=True)
    high = lax.Precision.HIGHEST
    cov = lax.dot_general(z, x, NT, precision=high, preferred_element_type=f32) / F
    vz = jnp.mean(z * z, axis=1, keepdims=True)
    ones = jnp.ones((8, F), f32)
    vx = lax.dot_general(ones, x * x, NT, precision=high, preferred_element_type=f32)[0:1] / F
    out[...] = jnp.where(alive, cov / jnp.sqrt((vx + epsilon) * (vz + epsilon)), 0.0)


def row_select(n, first):
    j5 = iota((5 * n, 16), 1)
    r5 = iota((5 * n, 16), 0)
    s5 = j5 - 3 * (r5 >> 4)
    k5 = (r5 & 15) + first
    fits = (s5 >= 0) & (s5 < 3)

    def select(d):
        return hot(fits & (k5 == 3 * d + s5))

    return select


def before_kernel(
    comp, foot_in, tr_in, geo_in, wide, merged, mtrace, oxa, oxb, oya, oyb, rxa, rxb,
    base, tbase, upper, lower, corr, foot, tr, geo, sem,
):
    quick = begin((geo_in, geo, sem.at[0]))
    ready = begin((tr_in, tr, sem.at[1]), (foot_in, foot, sem.at[2]))
    _, _, sy, sx = sides()
    n = 16
    whole, tail = receive_sides(row_select(n, 8), n, (rxa, rxb), sx, geo, quick)
    flag = tail[:, CH : CH + 1] > 0.5
    k = iota((n, 1), 0) + 8
    x_lo = jnp.where(k >= 12, PW - geo[0, 3], 0)
    x_hi = jnp.where(flag, jnp.where(k < 12, geo[0, 2], PW), 0)
    x = iota((1, CH), 1) & (PW - 1)
    inside = (x >= x_lo) & (x < x_hi)
    own_hot = hot(iota((K - BORDER, MP), 0) + BORDER == wide[0:1, 0:MP])
    hit = jnp.sum(own_hot.astype(f32), axis=1, keepdims=True) > 0.5
    ready()
    correlate(iota((1, K), 1) < comp[0, 0], tr[...], oxa, oxb, oya, oyb, corr, sy, sx)
    alive = iota((K - BORDER, 1), 0) + BORDER < comp[0, 0]
    step = 512
    for b in range(NPIX // step):
        lanes = slice(step * b, step * (b + 1))
        mine = foot[:, lanes].astype(f32)
        got = dot(own_hot, merged[:, lanes])
        low = jnp.where(alive, jnp.where(hit, got, mine[BORDER:]), 0.0)
        mid = []
        for q in range(step // CH):
            m = b * (step // CH) + q
            mid.append(
                jnp.where(
                    inside, whole[n * m : n * (m + 1)], mine[8:BORDER, CH * q : CH * (q + 1)]
                )
            )
        mid = jnp.concatenate(mid, axis=1)
        base[:, lanes] = jnp.concatenate([mine[0:8], mid, low], axis=0).astype(bf16)
        if step * b < BAND:
            upper[:, lanes] = jnp.concatenate([mine[0:8], mid[0:8]], axis=0)
        if step * b >= LOW:
            lower[:, step * b - LOW : step * (b + 1) - LOW] = mid
    mine = tr[...].astype(f32)
    mid = jnp.where(flag, tail[:, 0:F], mine[8:BORDER])
    low = jnp.where(alive, jnp.where(hit, dot(own_hot, mtrace[...]), mine[BORDER:]), 0.0)
    tbase[...] = jnp.concatenate([mine[0:8], mid, low], axis=0)


def final_kernel(
    geo_in, base, tbase, upper, lower, rya, ryb,
    nfoot, ntrace, placed, tails, pbuf, out, tout, geo, sem,
):
    ready = begin((geo_in, geo, sem.at[0]))
    _, _, sy, sx = sides()
    n = 16
    downs = [jnp.where(sy[u] > 0, 1, 0) for u in range(2)]
    bands = receive_bands(
        [row_select(n, 8 * dn) for dn in downs], n, (rya, ryb), pbuf, sy, sx, geo, ready
    )
    for dn, (moved, tail) in zip(downs, bands):
        for m in range(12):
            placed[dn, :, CH * m : CH * (m + 1)] = moved[n * m : n * (m + 1)]
        tails[dn] = tail
    mine = tbase[0:BORDER]
    gap = jnp.zeros((8, 2 * CH), f32)
    both = jnp.concatenate([tails[0], gap], axis=0) + jnp.concatenate([gap, tails[1]], axis=0)
    top = jnp.where(both[:, CH : CH + 1] > 0.5, both[:, 0:F], mine)
    tout[...] = jnp.concatenate([top, tbase[BORDER:]], axis=0).astype(bf16)
    copies = [pltpu.make_async_copy(tout, ntrace, sem.at[1])]
    copies[0].start()
    r_up, r_dn, c_lf, c_rt = (geo[0, i] for i in range(4))
    k = iota((n, 1), 0)
    pix = iota((1, BAND), 1)
    y = pix >> 6
    x = pix & (PW - 1)
    for dn, edge in enumerate((upper, lower)):
        j = k - 7 * dn
        flag = tails[dn, :, CH : CH + 1] > 0.5
        x_lo = jnp.where(j >= 6, PW - c_rt, 0)
        x_hi = jnp.where(flag, jnp.where(j < 3, c_lf, PW), 0)
        y_ok = (y < r_up) if dn == 0 else (y >= OV_HI - r_dn)
        inside = y_ok & (x >= x_lo) & (x < x_hi)
        out[dn] = jnp.where(inside, placed[dn], edge[...]).astype(bf16)
        copies.append(
            pltpu.make_async_copy(
                out.at[dn],
                nfoot.at[8 * dn : 8 * dn + 16, LOW * dn : LOW * dn + BAND],
                sem.at[2 + dn],
            )
        )
        copies[-1].start()
    for copy in copies:
        copy.wait()


SMEM = pl.BlockSpec(memory_space=pltpu.SMEM)
VMEM = pl.BlockSpec(memory_space=pltpu.VMEM)
LIMIT = 24 * 1024 * 1024


def shape(*dims, dtype=bf16):
    return jax.ShapeDtypeStruct(dims, dtype)


PACKETS = (shape(16, XW), shape(16, XW), shape(16, CW), shape(16, CW))
HBM = pl.BlockSpec(memory_space=pltpu.HBM)


def call(kernel, outs, ins, out_specs, scratch, flops, aliases={}):
    return pl.pallas_call(
        kernel,
        out_shape=outs,
        in_specs=ins,
        out_specs=out_specs,
        scratch_shapes=scratch,
        input_output_aliases=aliases,
        compiler_params=pltpu.CompilerParams(vmem_limit_bytes=LIMIT),
        cost_estimate=pl.CostEstimate(flops=flops, bytes_accessed=1 << 20, transcendentals=0),
    )


def swap(value, axis, parity):
    count = lax.axis_size(axis)
    pairs = []
    for i in range(parity, count - 1, 2):
        pairs += [(i, i + 1), (i + 1, i)]
    return lax.ppermute(value, axis, pairs)


def exchange(xa, xb, va, vb):
    rxb = swap(xb, "px", 1)
    rxa = swap(xa, "px", 0)
    yb = jnp.concatenate([vb, rxa[:, CW : 2 * CW], rxb[:, CW : 2 * CW]], axis=1)
    ya = jnp.concatenate([va, rxa[:, 0:CW], rxb[:, 0:CW]], axis=1)
    ryb = swap(yb, "py", 1)
    rya = swap(ya, "py", 0)
    return rxa, rxb, rya, ryb


def body(
    residual, footprints, traces, merge_pairs, pair_counts, comp_counts, row_inter, col_inter
):
    res = residual[0, 0]
    foot = footprints[0, 0]
    tr = traces[0, 0]
    table = merge_pairs[0, 0]
    wide = jnp.tile(table.T, (1, CH // MP))
    rows, cols = lax.axis_size("py"), lax.axis_size("px")
    res, foot, tr, row_far, col_far = (
        pltpu.with_memory_space_constraint(v, pltpu.HBM)
        for v in (res, foot, tr, row_inter, col_inter)
    )
    dma = pltpu.SemaphoreType.DMA
    i32 = jnp.int32
    geo_scratch = [pltpu.SMEM((1, CH), i32), dma((1,))]

    packets = call(
        pack_kernel,
        PACKETS,
        [HBM] * 2,
        (VMEM,) * 4,
        [pltpu.VMEM((32, NPIX), bf16), pltpu.VMEM((32, F), bf16), dma((2,))],
        1 << 24,
    )(foot, tr)
    rxa, rxb, rya, ryb = exchange(*packets)

    def own(*refs):
        own_kernel(rows, cols, *refs)

    def part(size):
        return (shape(size, F), shape(F, size), shape(MP, size, dtype=f32))

    *prepared, geo = call(
        own,
        part(HEAD)
        + (
            shape(MP, F, dtype=f32),
            shape(1, CH, dtype=i32),
        ),
        [HBM] * 4 + [VMEM],
        (VMEM,) * 5,
        [
            pltpu.VMEM((K, F), bf16),
            pltpu.SMEM((rows - 1,), i32),
            pltpu.SMEM((cols - 1,), i32),
            dma((3,)),
            dma((HEAD // 512,)),
        ],
        1 << 24,
    )(row_far, col_far, res, tr, table)

    *placed, slots, across = call(
        side_kernel,
        part(NPIX - HEAD)
        + (
            shape(MP, NPIX, dtype=f32),
            shape(MP, NPIX, dtype=f32),
            shape(MP, F, dtype=f32),
            shape(MP, CH, dtype=i32),
            shape(8, CH, dtype=i32),
        ),
        [SMEM] + [HBM] * 2 + [VMEM] * 6,
        (VMEM,) * 8,
        [pltpu.VMEM((K, NPIX), bf16), pltpu.SMEM((1, CH), i32), dma((2,)), dma(((NPIX - HEAD) // 512,))],
        1 << 24,
    )(pair_counts, res, foot, geo, prepared[-1], table, wide, rxa, rxb)

    xa, xb, va, vb, merged, mtrace = call(
        refit_kernel,
        PACKETS + (shape(MP, NPIX), shape(MP, F)),
        [VMEM] * 15,
        (VMEM,) * 6,
        [pltpu.VMEM((MP, NPIX), f32), pltpu.VMEM((6, MP, PBW), bf16)] + geo_scratch,
        1 << 28,
    )(geo, *prepared, slots, across, *placed, rya, ryb)
    oxa, oxb, oya, oyb = exchange(xa, xb, va, vb)

    *partial, corr = call(
        before_kernel,
        (
            shape(K, NPIX),
            shape(K, F, dtype=f32),
            shape(16, BAND, dtype=f32),
            shape(16, BAND, dtype=f32),
            shape(BORDER, K, dtype=f32),
        ),
        [SMEM] + [HBM] * 2 + [VMEM] * 10,
        (VMEM,) * 5,
        [
            pltpu.VMEM((K, NPIX), bf16),
            pltpu.VMEM((K, F), bf16),
            pltpu.SMEM((1, CH), i32),
            dma((3,)),
        ],
        1 << 24,
    )(comp_counts, foot, tr, geo, across, merged, mtrace, rxa, rxb, rya, ryb, oxa, oxb)

    nfoot, ntrace = call(
        final_kernel,
        (shape(K, NPIX), shape(K, F)),
        [VMEM, HBM] + [VMEM] * 5,
        (HBM, HBM),
        [
            pltpu.VMEM((2, 16, BAND), f32),
            pltpu.VMEM((2, 16, 2 * CH), f32),
            pltpu.VMEM((6, 16, PBW), bf16),
            pltpu.VMEM((2, 16, BAND), bf16),
            pltpu.VMEM((K, F), bf16),
            pltpu.SMEM((1, CH), i32),
            dma((4,)),
        ],
        1 << 26,
        {1: 0},
    )(geo, *partial, oya, oyb)
    return nfoot[None, None], ntrace[None, None], corr.T[None, None]


def solution(mesh):
    in_specs = (
        P("py", "px", None, None),
        P("py", "px", None, None),
        P("py", "px", None, None),
        P("py", "px", None, None),
        P("py", "px"),
        P("py", "px"),
        P(),
        P(),
    )
    out_specs = (P("py", "px", None, None), P("py", "px", None, None), P("py", "px", None, None))
    return jax.shard_map(body, mesh=mesh, in_specs=in_specs, out_specs=out_specs, check_vma=False)
```
